32 devices in a mesh: batch: 4 (over y, x), cols: 8 (over z, core).
Axes of the slice: x: 2, y: 2, z: 4, core: 2. Of those that a mesh axis runs over, the one named last changes fastest.
Arguments:
- grad_query: float32 [4, 2048, 2048], P('batch', None, 'cols'), may hold values from -0.875 to 0.875
- grad_key: float32 [4, 2048, 2048], P('batch', None, 'cols'), may hold values from -0.875 to 0.875
- grad_value: float32 [4, 2048, 2048], P('batch', None, 'cols'), may hold values from -0.875 to 0.875
- grad_mixed: float32 [4, 2048, 2048], P('batch', 'cols'), may hold values from -0.875 to 0.875
- grad_norm: float32 [4, 2048], P('batch'), may hold values from -8 to 8
- grad_bias: float32 [4, 2048], P('batch'), may hold values from -8 to 8
- weight_query: float32 [2048, 2048], P('batch', 'cols'), may hold values from -0.1875 to 0.1875
- weight_key: float32 [2048, 2048], P('batch', 'cols'), may hold values from -0.1875 to 0.1875
- weight_value: float32 [2048, 2048], P('batch', 'cols'), may hold values from -0.1875 to 0.1875
- weight_mixed: float32 [2048, 2048], P('cols', 'batch'), may hold values from -0.1875 to 0.1875
- weight_norm: float32 [2048], P('batch'), may hold values from 0.25 to 1.75
- weight_bias: float32 [2048], P('batch'), may hold values from -3 to 3
Outputs:
- copy_query: bfloat16 [2048, 2048], P(None, 'cols')
- copy_key: bfloat16 [2048, 2048], P(None, 'cols')
- copy_value: bfloat16 [2048, 2048], P(None, 'cols')
- copy_mixed: bfloat16 [2048, 2048], P('cols')
- copy_norm: bfloat16 [2048], replicated
- copy_bias: bfloat16 [2048], replicated
- new_query: float32 [2048, 2048], P('batch', 'cols')
- new_key: float32 [2048, 2048], P('batch', 'cols')
- new_value: float32 [2048, 2048], P('batch', 'cols')
- new_mixed: float32 [2048, 2048], P('cols', 'batch')
- new_norm: float32 [2048], P('batch')
- new_bias: float32 [2048], P('batch')
The draws below stay inside these ranges and needn't reach their ends.
All inputs are finite; a program needn't handle non-finite values.
Results may differ from the reference program's by a relative error of at most 0.0004.
Values may be sent and summed in bfloat16 or wider, within the bound.
A program may use at most 64 MiB of HBM per device.

```python
import jax
import jax.numpy as jnp
from jax import lax

WIDTH = 2048
ATTN = 2048
REPLICAS = 4


def strengthened(entries, own_key, source, target, shards_of, factor):
    owner, partner = [(jnp.arange(entries.shape[position]) // (entries.shape[position] // shards_of)).reshape([-1 if axis == position else 1 for axis in range(entries.ndim)]) for position in (source, target)]
    chosen = jax.random.permutation(own_key, shards_of)[partner]
    strong = (owner == chosen) | (owner == (partner + shards_of // 2) % shards_of)
    return jnp.where(strong, factor * entries, entries)


def block_scale(key, shape, split, low, largest):
    level, own = 1.0, jax.random.fold_in(key, 6)
    for position, parts in split:
        steps = jnp.exp(jax.random.uniform(jax.random.fold_in(own, position), (parts,), jnp.float32, low / len(split), largest / len(split)))
        level = level * jnp.repeat(steps, shape[position] // parts).reshape([-1 if axis == position else 1 for axis in range(len(shape))])
    return level


def bell_draw(rng, extent, deviation, bound, cuts=(), held_as=jnp.bfloat16):
    values = jax.random.normal(rng, extent, jnp.float32) * deviation
    if len(cuts) > 0:
        values = block_scale(rng, extent, cuts, -0.22, 0.18) * values
    return jnp.clip(values, min=-bound, max=bound).astype(held_as)


def bell_draw_with(key, shape, deviation, most, split, heavy, held_as=jnp.bfloat16):
    entries = deviation * jax.random.normal(key, shape, jnp.float32)
    if split:
        entries = entries * block_scale(key, shape, split, -0.22, 0.18)
    return jnp.clip(strengthened(entries, jax.random.fold_in(key, 3), *heavy), -most, most).astype(held_as)


def setup_inputs(seed: int = 0) -> dict:
    seeds = jax.random.split(jax.random.key(seed), 13)
    grad_query = bell_draw_with(seeds[0], (REPLICAS, WIDTH, ATTN), 0.1, 0.875, ((0, 4), (2, 8)), (0, 1, 4, 2.0), jnp.float32)
    grad_key = bell_draw_with(seeds[1], (REPLICAS, WIDTH, ATTN), 0.1, 0.875, ((0, 4), (2, 8)), (0, 1, 4, 2.0), jnp.float32)
    grad_value = bell_draw_with(seeds[2], (REPLICAS, WIDTH, ATTN), 0.1, 0.875, ((0, 4), (2, 8)), (0, 1, 4, 2.0), jnp.float32)
    grad_mixed = bell_draw_with(seeds[3], (REPLICAS, ATTN, WIDTH), 0.1, 0.875, ((0, 4), (1, 8)), (0, 2, 4, 2.0), jnp.float32)
    grad_norm = bell_draw_with(seeds[4], (REPLICAS, WIDTH), 1.0, 8.0, ((0, 4),), (0, 1, 4, 2.0), jnp.float32)
    grad_bias = bell_draw_with(seeds[5], (REPLICAS, WIDTH), 1.0, 8.0, ((0, 4),), (0, 1, 4, 2.0), jnp.float32)
    weight_query = bell_draw_with(seeds[6], (WIDTH, ATTN), WIDTH ** -0.5, 0.1875, ((0, 4), (1, 8)), (1, 0, 8, 2.0), jnp.float32)
    weight_key = bell_draw_with(seeds[7], (WIDTH, ATTN), WIDTH ** -0.5, 0.1875, ((0, 4), (1, 8)), (1, 0, 8, 2.0), jnp.float32)
    weight_value = bell_draw_with(seeds[8], (WIDTH, ATTN), WIDTH ** -0.5, 0.1875, ((0, 4), (1, 8)), (1, 0, 8, 2.0), jnp.float32)
    weight_mixed = bell_draw_with(seeds[9], (ATTN, WIDTH), ATTN ** -0.5, 0.1875, ((0, 8), (1, 4)), (0, 1, 8, 2.0), jnp.float32)
    weight_norm = jnp.clip(1.0 + 0.15 * jax.random.normal(seeds[10], (WIDTH,), jnp.float32), 0.25, 1.75)
    weight_bias = bell_draw(seeds[11], (WIDTH,), 0.5, 3.0, ((0, 4),), jnp.float32)
    return dict(grad_query=grad_query, grad_key=grad_key, grad_value=grad_value, grad_mixed=grad_mixed, grad_norm=grad_norm, grad_bias=grad_bias, weight_query=weight_query, weight_key=weight_key, weight_value=weight_value, weight_mixed=weight_mixed, weight_norm=weight_norm, weight_bias=weight_bias)


learn_rate = 0.4

def reference(grad_query, grad_key, grad_value, grad_mixed, grad_norm, grad_bias, weight_query, weight_key, weight_value, weight_mixed, weight_norm, weight_bias):
    mean_query = lax.optimization_barrier(jnp.sum(grad_query.astype(jnp.float32), axis=0)) * REPLICAS ** (-0.5)
    mean_key = lax.optimization_barrier(jnp.sum(grad_key.astype(jnp.float32), axis=0)) * REPLICAS ** (-0.5)
    mean_value = lax.optimization_barrier(jnp.sum(grad_value.astype(jnp.float32), axis=0)) * REPLICAS ** (-0.5)
    mean_mixed = lax.optimization_barrier(jnp.sum(grad_mixed.astype(jnp.float32), axis=0)) * REPLICAS ** (-0.5)
    mean_norm = lax.optimization_barrier(jnp.sum(grad_norm.astype(jnp.float32), axis=0)) * REPLICAS ** (-0.5)
    mean_bias = lax.optimization_barrier(jnp.sum(grad_bias.astype(jnp.float32), axis=0)) * REPLICAS ** (-0.5)
    ratio_query = jnp.sqrt(lax.optimization_barrier(jnp.sum(weight_query * weight_query, axis=1, keepdims=True))) * lax.rsqrt(lax.optimization_barrier(jnp.sum(mean_query * mean_query, axis=1, keepdims=True)) + 1e-06)
    mean_query = mean_query * ratio_query
    ratio_key = jnp.sqrt(lax.optimization_barrier(jnp.sum(weight_key * weight_key, axis=1, keepdims=True))) * lax.rsqrt(lax.optimization_barrier(jnp.sum(mean_key * mean_key, axis=1, keepdims=True)) + 1e-06)
    mean_key = mean_key * ratio_key
    ratio_value = jnp.sqrt(lax.optimization_barrier(jnp.sum(weight_value * weight_value, axis=1, keepdims=True))) * lax.rsqrt(lax.optimization_barrier(jnp.sum(mean_value * mean_value, axis=1, keepdims=True)) + 1e-06)
    mean_value = mean_value * ratio_value
    ratio_mixed = jnp.sqrt(lax.optimization_barrier(jnp.sum(weight_mixed * weight_mixed, axis=0, keepdims=True))) * lax.rsqrt(lax.optimization_barrier(jnp.sum(mean_mixed * mean_mixed, axis=0, keepdims=True)) + 1e-06)
    mean_mixed = mean_mixed * ratio_mixed
    new_query = weight_query - learn_rate * mean_query
    new_key = weight_key - learn_rate * mean_key
    new_value = weight_value - learn_rate * mean_value
    new_mixed = weight_mixed - learn_rate * mean_mixed
    new_norm = weight_norm - learn_rate * mean_norm
    new_bias = weight_bias - learn_rate * mean_bias
    copy_query = new_query.astype(jnp.bfloat16)
    copy_key = new_key.astype(jnp.bfloat16)
    copy_value = new_value.astype(jnp.bfloat16)
    copy_mixed = new_mixed.astype(jnp.bfloat16)
    copy_norm = new_norm.astype(jnp.bfloat16)
    copy_bias = new_bias.astype(jnp.bfloat16)
    return (copy_query, copy_key, copy_value, copy_mixed, copy_norm, copy_bias, new_query, new_key, new_value, new_mixed, new_norm, new_bias)
```

```python
import functools
import math

import jax
import jax.numpy as jnp
from jax import lax
from jax.experimental import pallas as pl
from jax.experimental.pallas import tpu as pltpu
from jax.sharding import PartitionSpec as P

learn_rate = 0.4
LANES = 128
LOW, SPAN, TINY = 87.0, 175.0, 1e-30
ORDER = (
    ("F0", "F1", "S", "W0", "W1", "W2", "W3", "A0", "F2", "A1", "F3", "N", "B0")
    + ("A2", "B1", "U0", "A3", "B2", "U1", "P0", "B3", "U2", "P1", "U3", "P2", "P3")
)


def kernel(n, m, n_x, n_y, *refs):
    grads, small_grads = refs[0:4], refs[4:6]
    weights, small_weights = refs[6:10], refs[10:12]
    copies, news = refs[12:16], refs[16:20]
    small_full, small_own = refs[20:22]
    scratch = refs[22:]
    first_in, second_in, held = scratch[0:4], scratch[4:8], scratch[8:12]
    total, own_weight = scratch[12:16], scratch[16:20]
    raw, first_out, second_out = scratch[20:24], scratch[24:28], scratch[28:32]
    first_unit, first_unit_in = scratch[32:36], scratch[36:40]
    second_unit, second_unit_in = scratch[40:44], scratch[44:48]
    squares, squares_in, small_in = scratch[48:51]
    (
        load_sem, raw_sem, weight_sem,
        first_send, first_recv, second_send, second_recv,
        first_unit_send, first_unit_recv, second_unit_send, second_unit_recv,
        square_send, square_recv, square_own,
        back_send, back_recv, spread_send, spread_recv,
        small_send, small_recv, small_local,
    ) = scratch[51:]
    rate = n ** (-0.5)

    me = lax.axis_index("batch")
    col = lax.axis_index("cols")
    y, x = me // n_x, lax.rem(me, n_x)

    def spot(half, d_first, d_second):
        if half == 0:
            return lax.rem(y + d_second, n_y) * n_x + lax.rem(x + d_first, n_x)
        return lax.rem(y + d_first, n_y) * n_x + lax.rem(x + d_second, n_x)

    def extents(half):
        return (n_x, n_y) if half == 0 else (n_y, n_x)

    def piece(a, ref, chunk, half):
        rows, columns = total[a].shape
        depth = rows // 2
        if a < 3:
            start = pl.multiple_of(chunk * rows + half * depth, depth)
            return ref.at[pl.ds(start, depth), :]
        start = pl.multiple_of(chunk * columns, columns)
        return ref.at[pl.ds(half * depth, depth), pl.ds(start, columns)]

    loads, raw_loads, weight_loads = {}, {}, []
    for a in range(4):
        for d in range(max(n_x, n_y) - 1, -1, -1):
            for half in range(2):
                n_first, n_second = extents(half)
                if d >= n_second:
                    continue
                for d_first in range(1, n_first):
                    raw_loads[a, half, d_first, d] = pltpu.make_async_copy(
                        piece(a, grads[a].at[0], spot(half, d_first, d), half),
                        raw[a].at[half, d_first - 1, d],
                        raw_sem.at[a, half, d_first - 1, d],
                    )
                loads[a, half, d] = pltpu.make_async_copy(
                    piece(a, grads[a].at[0], spot(half, 0, d), half),
                    held[a].at[half, d],
                    load_sem.at[a, half, d],
                )
        weight_loads.append(pltpu.make_async_copy(weights[a], own_weight[a], weight_sem.at[a]))
    small_loads, width = [], small_weights[0].shape[1]
    for i in range(2):
        small_loads.append(
            pltpu.make_async_copy(small_grads[i], small_in.at[me, :, pl.ds(i * n * width, n * width)], small_local.at[i])
        )
        small_loads.append(
            pltpu.make_async_copy(
                small_weights[i], small_in.at[me, :, pl.ds((2 * n + i) * width, width)], small_local.at[2 + i]
            )
        )

    barrier = pltpu.get_barrier_semaphore()
    for d in range(1, n):
        pl.semaphore_signal(barrier, inc=1, device_id={"batch": lax.rem(me + d, n)})
    for d in range(1, m):
        pl.semaphore_signal(barrier, inc=1, device_id={"cols": lax.rem(col + d, m)})
    for key, copy in raw_loads.items():
        if key[0] == 0:
            copy.start()
    for copy in small_loads:
        copy.start()
    for key, copy in raw_loads.items():
        if key[0] == 1:
            copy.start()
    for key, copy in loads.items():
        if key[0] < 2:
            copy.start()
    for copy in weight_loads:
        copy.start()
    for key, copy in raw_loads.items():
        if key[0] > 1:
            copy.start()
    for key, copy in loads.items():
        if key[0] > 1:
            copy.start()

    def across(a, line, depth):
        if a < 3:
            return jnp.broadcast_to(line, (LANES, depth)).T
        return line

    def blocks_of(a, columns):
        if a < 3:
            return [slice(start, start + LANES) for start in range(0, columns, LANES)]
        return [slice(0, columns)]

    def encode(a, source, code, unit):
        depth, columns = source.shape
        value = source[...]
        size = jnp.abs(value)
        if a < 3:
            folded = functools.reduce(jnp.maximum, [size[:, block] for block in blocks_of(a, columns)])
            size = folded.T
        most = jnp.maximum(jnp.max(size, axis=0, keepdims=True), TINY)
        unit[...] = most * SPAN**-2
        gain = across(a, SPAN**2 / most, depth)
        for block in blocks_of(a, columns):
            part = value[:, block]
            spread_out = jnp.abs(part) * gain
            level = jnp.exp(spread_out * lax.rsqrt(spread_out + TINY) - LOW)
            code[:, block] = jnp.where(part < 0, -level, level).astype(jnp.bfloat16)

    def decode(a, code, unit):
        depth, columns = code.shape
        scale = across(a, unit[...], depth)
        parts = []
        for block in blocks_of(a, columns):
            part = code[:, block].astype(jnp.float32)
            root = jnp.log(jnp.abs(part)) + LOW
            level = root * root * scale
            parts.append(jnp.where(part < 0, -level, level))
        return jnp.concatenate(parts, axis=1) if len(parts) > 1 else parts[0]

    first, small = {}, []
    entered = []

    def send_first(a):
        for d_second in range(max(n_x, n_y) - 1, -1, -1):
            ready = []
            for half in range(2):
                n_first, n_second = extents(half)
                if d_second >= n_second:
                    continue
                for d_first in range(1, n_first):
                    at = (half, d_first - 1, d_second)
                    raw_loads[a, half, d_first, d_second].wait()
                    encode(a, raw[a].at[at], first_out[a].at[at], first_unit[a].at[at])
                    to = {"batch": spot(half, d_first, 0)}
                    pair = (
                        pltpu.make_async_remote_copy(
                            src_ref=first_unit[a].at[at],
                            dst_ref=first_unit_in[a].at[at],
                            send_sem=first_unit_send.at[(a,) + at],
                            recv_sem=first_unit_recv.at[(a,) + at],
                            device_id=to,
                        ),
                        pltpu.make_async_remote_copy(
                            src_ref=first_out[a].at[at],
                            dst_ref=first_in[a].at[at],
                            send_sem=first_send.at[(a,) + at],
                            recv_sem=first_recv.at[(a,) + at],
                            device_id=to,
                        ),
                    )
                    if entered:
                        pair[0].start()
                        pair[1].start()
                    ready.append(pair)
                    first[a, half, d_first, d_second] = pair
            if not entered:
                entered.append(True)
                pl.semaphore_wait(barrier, n - 1 + m - 1)
                for pair in ready:
                    pair[0].start()
                    pair[1].start()

    def send_small():
        for copy in small_loads:
            copy.wait()
        for d in range(1, n):
            copy = pltpu.make_async_remote_copy(
                src_ref=small_in.at[me],
                dst_ref=small_in.at[me],
                send_sem=small_send.at[d - 1],
                recv_sem=small_recv.at[d - 1],
                device_id={"batch": lax.rem(me + d, n)},
            )
            copy.start()
            small.append(copy)

    def row_squares(a, value):
        value = value * value
        if a == 3:
            return jnp.sum(value, axis=0, keepdims=True)
        folded = value[:, :LANES]
        for start in range(LANES, value.shape[1], LANES):
            folded = folded + value[:, start : start + LANES]
        return jnp.sum(folded.T, axis=0, keepdims=True)

    def weigh(a):
        weight_loads[a].wait()
        squares[a, 0:1] = row_squares(a, own_weight[a][...])

    second = {}

    def add_first(a):
        for d_second in range(max(n_x, n_y) - 1, -1, -1):
            for half in range(2):
                n_first, n_second = extents(half)
                if d_second >= n_second:
                    continue
                loads[a, half, d_second].wait()
                value = held[a][half, d_second]
                for d_first in range(1, n_first):
                    for copy in first[a, half, d_first, d_second]:
                        copy.wait_recv()
                    at = (half, d_first - 1, d_second)
                    value = value + decode(a, first_in[a].at[at], first_unit_in[a].at[at])
                held[a][half, d_second] = value
                if d_second > 0:
                    at = (half, d_second - 1)
                    encode(a, held[a].at[half, d_second], second_out[a].at[at], second_unit[a].at[at])
                    to = {"batch": spot(half, 0, d_second)}
                    pair = (
                        pltpu.make_async_remote_copy(
                            src_ref=second_unit[a].at[at],
                            dst_ref=second_unit_in[a].at[at],
                            send_sem=second_unit_send.at[(a,) + at],
                            recv_sem=second_unit_recv.at[(a,) + at],
                            device_id=to,
                        ),
                        pltpu.make_async_remote_copy(
                            src_ref=second_out[a].at[at],
                            dst_ref=second_in[a].at[at],
                            send_sem=second_send.at[(a,) + at],
                            recv_sem=second_recv.at[(a,) + at],
                            device_id=to,
                        ),
                    )
                    pair[0].start()
                    pair[1].start()
                    second[a, half, d_second] = pair

    exchange = {}

    def add_second(a):
        depth = total[a].shape[0] // 2
        for half in range(2):
            value = held[a][half, 0]
            for d_second in range(1, extents(half)[1]):
                for copy in second[a, half, d_second]:
                    copy.wait_recv()
                at = (half, d_second - 1)
                value = value + decode(a, second_in[a].at[at], second_unit_in[a].at[at])
            total[a][half * depth : (half + 1) * depth] = value * rate
        squares[a, 1:2] = row_squares(a, total[a][...])
        own = pltpu.make_async_copy(squares.at[a], squares_in.at[a, col], square_own.at[a])
        exchange[a] = [own]
        for d in range(1, m):
            copy = pltpu.make_async_remote_copy(
                src_ref=squares.at[a],
                dst_ref=squares_in.at[a, col],
                send_sem=square_send.at[a, d - 1],
                recv_sem=square_recv.at[a, d - 1],
                device_id={"cols": lax.rem(col + d, m)},
            )
            copy.start()
            exchange[a].append(copy)
        own.start()

    back, spread = {}, {}

    def send_spread(a, half, d_second):
        n_first, n_second = extents(half)
        slab = piece(a, copies[a], spot(half, 0, n_second - d_second), half)
        for d_first in range(1, n_first):
            copy = pltpu.make_async_remote_copy(
                src_ref=slab,
                dst_ref=slab,
                send_sem=spread_send.at[a, half, d_first - 1, d_second],
                recv_sem=spread_recv.at[a, half, d_first - 1, d_second],
                device_id={"batch": spot(half, d_first, 0)},
            )
            copy.start()
            spread[a, half, d_first, d_second] = copy

    def update(a):
        exchange[a][0].wait()
        for copy in exchange[a][1:]:
            copy.wait_recv()
        both = squares_in[a, 0]
        for d in range(1, m):
            both = both + squares_in[a, d]
        ratio = learn_rate * (jnp.sqrt(both[0:1]) * lax.rsqrt(both[1:2] + 1e-06))
        rows, columns = total[a].shape
        if a < 3:
            ratio = jnp.broadcast_to(ratio, (LANES, rows)).T
            for start in range(0, columns, LANES):
                block = slice(start, start + LANES)
                news[a][:, block] = own_weight[a][:, block] - total[a][:, block] * ratio
        else:
            news[a][...] = own_weight[a][...] - total[a][...] * ratio
        depth = rows // 2
        for half in range(2):
            piece(a, copies[a], me, half)[...] = news[a][half * depth : (half + 1) * depth].astype(jnp.bfloat16)
        for half in range(2):
            slab = piece(a, copies[a], me, half)
            for d_second in range(1, extents(half)[1]):
                copy = pltpu.make_async_remote_copy(
                    src_ref=slab,
                    dst_ref=slab,
                    send_sem=back_send.at[a, half, d_second - 1],
                    recv_sem=back_recv.at[a, half, d_second - 1],
                    device_id={"batch": spot(half, 0, d_second)},
                )
                copy.start()
                back[a, half, d_second] = copy
            send_spread(a, half, 0)

    def pass_on(a):
        for half in range(2):
            for d_second in range(1, extents(half)[1]):
                back[a, half, d_second].wait_recv()
                send_spread(a, half, d_second)

    def update_small():
        for copy in small:
            copy.wait()
        for i in range(2):
            value = small_in[0, :, i * n * width : (i + 1) * n * width]
            for j in range(1, n):
                value = value + small_in[j, :, i * n * width : (i + 1) * n * width]
            value = value * rate
            for j in range(n):
                weight = small_in[j, :, (2 * n + i) * width : (2 * n + i + 1) * width]
                small_full[i, j] = weight - learn_rate * value[:, j * width : (j + 1) * width]
            small_own[i] = small_full[i, me]

    steps = dict(
        F=send_first, S=send_small, W=weigh, A=add_first, N=update_small, B=add_second, U=update, P=pass_on
    )
    for step in ORDER:
        steps[step[0]](*map(int, step[1:]))
    for pairs in (first, second):
        for pair in pairs.values():
            pair[0].wait_send()
            pair[1].wait_send()
    for copies_sent in (back, spread):
        for copy in copies_sent.values():
            copy.wait_send()
    for a in range(4):
        for copy in exchange[a][1:]:
            copy.wait_send()
    for copy in spread.values():
        copy.wait_recv()


def finish(n, *refs):
    results, full, own = refs[0:8], refs[8], refs[9]
    outs, small_copies, small_news = refs[10:18], refs[18:20], refs[20:22]
    copy_rows, new_rows, sem, small_sem = refs[22:24], refs[24:26], refs[26], refs[27]
    moves = [pltpu.make_async_copy(results[i], outs[i], sem.at[i]) for i in range(8)]
    for move in moves:
        move.start()
    width = full.shape[-1]
    for i in range(2):
        for j in range(n):
            copy_rows[i][j * width : (j + 1) * width] = full[i, j, 0].astype(jnp.bfloat16)
        new_rows[i][...] = own[i, 0]
    for i in range(2):
        moves.append(pltpu.make_async_copy(copy_rows[i], small_copies[i], small_sem.at[i]))
        moves.append(pltpu.make_async_copy(new_rows[i], small_news[i], small_sem.at[2 + i]))
    for move in moves[8:]:
        move.start()
    for move in moves:
        move.wait()


def solution(mesh):
    n, m = mesh.shape["batch"], mesh.shape["cols"]
    n_x = math.isqrt(n)
    if n_x * n_x != n:
        n_x = n
    n_y = n // n_x
    most = max(n_x, n_y)

    def per_device(*args):
        args = args[:10] + tuple(w.reshape(1, -1) for w in args[10:])
        grads, weights, width = args[0:4], args[6:10], args[10].shape[1]
        blocks = [w.shape for w in weights]
        slices = blocks[0][0]
        slabs = [(b[0] // 2, b[1]) for b in blocks]
        lines = [(1, s[0]) for s in slabs[:3]] + [(1, slabs[3][1])]
        f32, bf16 = jnp.float32, jnp.bfloat16
        DMA = pltpu.SemaphoreType.DMA
        hops = max(most - 1, 1)
        hbm = pl.BlockSpec(memory_space=pltpu.HBM)
        vmem = pl.BlockSpec(memory_space=pltpu.VMEM)
        out_shape = (
            [jax.ShapeDtypeStruct(g.shape[1:], bf16) for g in grads]
            + [jax.ShapeDtypeStruct(b, f32) for b in blocks]
            + [jax.ShapeDtypeStruct((2, n, 1, width), f32), jax.ShapeDtypeStruct((2, 1, width), f32)]
        )
        results = pl.pallas_call(
            functools.partial(kernel, n, m, n_x, n_y),
            out_shape=[pltpu.VMEM(o.shape, o.dtype) for o in out_shape],
            in_specs=[hbm] * 12,
            out_specs=[vmem] * 10,
            scratch_shapes=(
                [pltpu.VMEM((2, hops, most) + s, bf16) for s in slabs]
                + [pltpu.VMEM((2, hops) + s, bf16) for s in slabs]
                + [pltpu.VMEM((2, most) + s, f32) for s in slabs]
                + [pltpu.VMEM(b, f32) for b in blocks]
                + [pltpu.VMEM(b, f32) for b in blocks]
                + [pltpu.VMEM((2, hops, most) + s, f32) for s in slabs]
                + [pltpu.VMEM((2, hops, most) + s, bf16) for s in slabs]
                + [pltpu.VMEM((2, hops) + s, bf16) for s in slabs]
                + [pltpu.VMEM((2, hops, most) + l, f32) for l in lines] * 2
                + [pltpu.VMEM((2, hops) + l, f32) for l in lines] * 2
                + [
                    pltpu.VMEM((4, 2, slices), f32),
                    pltpu.VMEM((4, m, 2, slices), f32),
                    pltpu.VMEM((n, 1, 2 * (n + 1) * width), f32),
                    DMA((4, 2, most)),
                    DMA((4, 2, hops, most)),
                    DMA((4,)),
                    DMA((4, 2, hops, most)),
                    DMA((4, 2, hops, most)),
                    DMA((4, 2, hops)),
                    DMA((4, 2, hops)),
                    DMA((4, 2, hops, most)),
                    DMA((4, 2, hops, most)),
                    DMA((4, 2, hops)),
                    DMA((4, 2, hops)),
                    DMA((4, m)),
                    DMA((4, m)),
                    DMA((4,)),
                    DMA((4, 2, hops)),
                    DMA((4, 2, hops)),
                    DMA((4, 2, hops, most)),
                    DMA((4, 2, hops, most)),
                    DMA((n,)),
                    DMA((n,)),
                    DMA((4,)),
                ]
            ),
            compiler_params=pltpu.CompilerParams(
                collective_id=0, has_side_effects=True, vmem_limit_bytes=40 * 2**20
            ),
        )(*[pltpu.with_memory_space_constraint(v, pltpu.HBM) for v in args])
        done = pl.pallas_call(
            functools.partial(finish, n),
            out_shape=out_shape[:8]
            + [jax.ShapeDtypeStruct((n * width,), bf16)] * 2
            + [jax.ShapeDtypeStruct((width,), f32)] * 2,
            in_specs=[vmem] * 10,
            out_specs=[hbm] * 12,
            scratch_shapes=[pltpu.VMEM((n * width,), bf16)] * 2
            + [pltpu.VMEM((width,), f32)] * 2
            + [DMA((8,)), DMA((4,))],
            compiler_params=pltpu.CompilerParams(vmem_limit_bytes=2**20),
        )(*results)
        return tuple(done[0:4]) + tuple(done[8:10]) + tuple(done[4:8]) + tuple(done[10:12])

    in_specs = (
        (P("batch", None, "cols"),) * 3
        + (P("batch", "cols", None),)
        + (P("batch", None),) * 2
        + (P("batch", "cols"),) * 3
        + (P("cols", "batch"),)
        + (P("batch"),) * 2
    )
    out_specs = (
        (P(None, "cols"),) * 3
        + (P("cols", None),)
        + (P(),) * 2
        + (P("batch", "cols"),) * 3
        + (P("cols", "batch"),)
        + (P("batch"),) * 2
    )
    return jax.shard_map(per_device, mesh=mesh, in_specs=in_specs, out_specs=out_specs, check_vma=False)
```

```python
import functools
import math

import jax
import jax.numpy as jnp
from jax import lax
from jax.experimental import pallas as pl
from jax.experimental.pallas import tpu as pltpu
from jax.sharding import PartitionSpec as P

learn_rate = 0.4
LANES = 128
LOW, SPAN, TINY = 87.0, 175.0, 1e-30
ORDER = (
    ("F0", "F1", "W0", "W1", "W2", "W3", "A0", "S", "F2", "A1", "F3", "E", "N", "B0")
    + ("A2", "B1", "U0", "A3", "B2", "U1", "P0", "M", "B3", "U2", "P1", "U3", "P2", "P3")
)


def across(a, line, depth):
    return jnp.broadcast_to(line, (LANES, depth)).T if a < 3 else line


def blocks_of(a, columns):
    step = LANES if a < 3 else columns
    return [slice(start, start + step) for start in range(0, columns, step)]


def encode(a, value, code, unit):
    depth, columns = value.shape
    size = jnp.abs(value)
    if a < 3:
        size = functools.reduce(jnp.maximum, [size[:, block] for block in blocks_of(a, columns)]).T
    largest = jnp.maximum(jnp.max(size, axis=0, keepdims=True), TINY)
    unit[...] = largest * SPAN**-2
    gain = across(a, SPAN**2 / largest, depth)
    for block in blocks_of(a, columns):
        part = value[:, block]
        level = jnp.abs(part) * gain
        level = jnp.exp(level * lax.rsqrt(level + TINY) - LOW)
        code[:, block] = jnp.where(part < 0, -level, level).astype(jnp.bfloat16)


def decode(a, code, unit):
    depth, columns = code.shape
    scale = across(a, unit[...], depth)
    parts = []
    for block in blocks_of(a, columns):
        part = code[:, block].astype(jnp.float32)
        root = jnp.log(jnp.abs(part)) + LOW
        level = root * root * scale
        parts.append(jnp.where(part < 0, -level, level))
    return jnp.concatenate(parts, axis=1) if len(parts) > 1 else parts[0]


def drain(ref, sem):
    pltpu.make_async_copy(ref, ref, sem).wait()


def kernel(n, m, n_x, n_y, *refs):
    grads, small_grads = refs[0:4], refs[4:6]
    weights, small_weights = refs[6:10], refs[10:12]
    copies, news = refs[12:16], refs[16:20]
    small_full, small_own = refs[20:22]
    scratch = refs[22:]
    full, total, own_weight = scratch[0:4], scratch[4:8], scratch[8:12]
    first_out, first_in = scratch[12:16], scratch[16:20]
    second_out, second_in = scratch[20:24], scratch[24:28]
    unit_out, first_unit, second_unit = scratch[28:32], scratch[32:36], scratch[36:40]
    squares, squares_in, small_hold, small_in, small_done = scratch[40:45]
    (
        early_sem, load_sem, weight_sem, small_local,
        send_sem, unit_send,
        first_recv, first_unit_recv, second_recv, second_unit_recv,
        square_send, square_recv, back_recv, spread_recv,
        small_sem, done_sem, plane_sem, row_sem,
    ) = scratch[45:]
    rate = n ** (-0.5)
    most = max(n_x, n_y)

    me = lax.axis_index("batch")
    col = lax.axis_index("cols")
    y, x = me // n_x, lax.rem(me, n_x)

    def spot(half, d_first, d_second):
        if half == 0:
            return lax.rem(y + d_second, n_y) * n_x + lax.rem(x + d_first, n_x)
        return lax.rem(y + d_first, n_y) * n_x + lax.rem(x + d_second, n_x)

    def extents(half):
        return (n_x, n_y) if half == 0 else (n_y, n_x)

    def piece(a, ref, chunk, half):
        rows, columns = total[a].shape
        depth = rows // 2
        if a < 3:
            start = pl.multiple_of(chunk * rows + half * depth, depth)
            return ref.at[pl.ds(start, depth), :]
        start = pl.multiple_of(chunk * columns, columns)
        return ref.at[pl.ds(half * depth, depth), pl.ds(start, columns)]

    def slots(a, ref, half):
        n_first, n_second = extents(half)
        return ref[a].at[half, pl.ds(0, n_first - 1), pl.ds(0, n_second)]

    odd = lax.rem(col, 2)
    pair = col - odd
    barrier = pltpu.get_barrier_semaphore()

    def greet(skip, **device):
        @pl.when(jnp.logical_not(skip))
        def _():
            pl.semaphore_signal(barrier, inc=1, device_id=device)

    neighbours = [spot(0, d, 0) for d in range(1, n_x)] + [spot(0, 0, d) for d in range(1, n_y)]
    for other in neighbours:
        pl.semaphore_signal(barrier, inc=1, device_id={"batch": other, "cols": pair})
    greet(odd == 0, batch=me, cols=pair)
    for d in range(0, m, 2):
        other = lax.rem(pair + d, m) + 1
        greet(other == col, batch=me, cols=other)

    def enter_plane():
        @pl.when(odd == 0)
        def _():
            pl.semaphore_wait(barrier, 2 * len(neighbours) + 1)
            pl.semaphore_signal(plane_sem, inc=1, device_id={"cols": col + 1})

        @pl.when(odd == 1)
        def _():
            pl.semaphore_wait(plane_sem, 1)

    def enter_row():
        @pl.when(odd == 1)
        def _():
            pl.semaphore_wait(barrier, m - 1)
            pl.semaphore_signal(row_sem, inc=1, device_id={"cols": col - 1})

        @pl.when(odd == 0)
        def _():
            pl.semaphore_wait(row_sem, 1)

    early, rest = {}, []
    for half in range(2):
        n_first, n_second = extents(half)
        for d_first in range(n_first):
            for d_second in range(n_second):
                here = spot(half, d_first, d_second)
                first_sent = d_first > 0 and d_second == n_second - 1
                copy = pltpu.make_async_copy(
                    piece(0, grads[0].at[0], here, half),
                    piece(0, full[0], here, half),
                    early_sem.at[half, d_first - 1] if first_sent else load_sem.at[0],
                )
                if first_sent:
                    early[half, d_first] = copy
                else:
                    rest.append(copy)
    width = small_weights[0].shape[1]
    shares, chunk = small_done.shape[0], small_done.shape[3]
    per_array = shares // 2
    share = lax.rem(col, shares)
    smalls, weight_loads = [], []
    for i in range(2):
        smalls.append((small_grads[i], small_hold.at[i, :, pl.ds(0, n * width)]))
        smalls.append((small_weights[i], small_hold.at[i, :, pl.ds(n * width, width)]))
    for copy in early.values():
        copy.start()
    for copy in rest:
        copy.start()
    for a in range(1, 4):
        pltpu.make_async_copy(grads[a].at[0], full[a], load_sem.at[a]).start()
        if a == 1:
            for b in range(4):
                weight_loads.append(pltpu.make_async_copy(weights[b], own_weight[b], weight_sem.at[b]))
                weight_loads[b].start()
            for source, target in smalls:
                pltpu.make_async_copy(source, target, small_local).start()

    def load_rest(a):
        if a == 0:
            drain(full[0].at[pl.ds(0, len(rest) * (total[0].shape[0] // 2))], load_sem.at[0])
        else:
            drain(full[a], load_sem.at[a])

    entered, loaded = [], set()

    def send(source, target, sem, arrival, device):
        pltpu.make_async_remote_copy(
            src_ref=source, dst_ref=target, send_sem=sem, recv_sem=arrival, device_id=device
        ).start()

    def send_first(a):
        for d in range(most - 1, -1, -1):
            for half in range(2):
                n_first, n_second = extents(half)
                for d_first in range(1, n_first):
                    if d >= n_second:
                        continue
                    if a == 0 and d == n_second - 1:
                        early[half, d_first].wait()
                    elif a not in loaded:
                        loaded.add(a)
                        load_rest(a)
                    at = (half, d_first - 1, d)
                    unit = unit_out[a].at[at]
                    encode(a, piece(a, full[a], spot(half, d_first, d), half)[...], first_out[a].at[at], unit)
                    if not entered:
                        entered.append(True)
                        enter_plane()
                    to = {"batch": spot(half, d_first, 0)}
                    send(unit, first_unit[a].at[at], unit_send.at[a], first_unit_recv.at[a], to)
                    send(first_out[a].at[at], first_in[a].at[at], send_sem.at[a], first_recv.at[a], to)

    def send_small():
        drain(small_hold, small_local)
        start = lax.rem(share, per_array) * chunk
        for k in range(n + 1):
            small_in[me, k] = small_hold[share // per_array, :, pl.ds(pl.multiple_of(k * width + start, chunk), chunk)]
        for d in range(1, n):
            send(small_in.at[me], small_in.at[me], small_sem.at[0], small_sem.at[1], {"batch": lax.rem(me + d, n)})

    def row_squares(a, value):
        value = value * value
        if a == 3:
            return jnp.sum(value, axis=0, keepdims=True)
        folded = value[:, :LANES]
        for start in range(LANES, value.shape[1], LANES):
            folded = folded + value[:, start : start + LANES]
        return jnp.sum(folded.T, axis=0, keepdims=True)

    def weigh(a):
        weight_loads[a].wait()
        squares[a, 0:1] = row_squares(a, own_weight[a][...])

    def drain_first(a, ref, sem):
        if n_x == n_y:
            drain(ref[a], sem)
        else:
            for half in range(2):
                if extents(half)[0] > 1:
                    drain(slots(a, ref, half), sem)

    def add_first(a):
        if a not in loaded:
            loaded.add(a)
            load_rest(a)
        drain_first(a, first_unit, first_unit_recv.at[a])
        drain_first(a, first_in, first_recv.at[a])
        for d_second in range(most - 1, -1, -1):
            for half in range(2):
                n_first, n_second = extents(half)
                if d_second >= n_second:
                    continue
                own = piece(a, full[a], spot(half, 0, d_second), half)
                value = own[...]
                for d_first in range(1, n_first):
                    at = (half, d_first - 1, d_second)
                    value = value + decode(a, first_in[a].at[at], first_unit[a].at[at])
                if d_second == 0:
                    own[...] = value
                    continue
                at = (half, d_second - 1)
                unit = unit_out[a].at[at + (most,)]
                encode(a, value, second_out[a].at[at], unit)
                to = {"batch": spot(half, 0, d_second)}
                send(unit, second_unit[a].at[at], unit_send.at[a], second_unit_recv.at[a], to)
                send(second_out[a].at[at], second_in[a].at[at], send_sem.at[a], second_recv.at[a], to)

    def used_second(a, ref):
        if n_x == n_y:
            return ref[a]
        half = 0 if n_y > 1 else 1
        return ref[a].at[half, pl.ds(0, extents(half)[1] - 1)]

    def add_second(a):
        drain(used_second(a, second_unit), second_unit_recv.at[a])
        drain(used_second(a, second_in), second_recv.at[a])
        depth = total[a].shape[0] // 2
        for half in range(2):
            value = piece(a, full[a], me, half)[...]
            for d_second in range(1, extents(half)[1]):
                at = (half, d_second - 1)
                value = value + decode(a, second_in[a].at[at], second_unit[a].at[at])
            total[a][half * depth : (half + 1) * depth] = value * rate
        squares[a, 1:2] = row_squares(a, total[a][...])
        squares_in[a, col] = squares[a]
        for d in range(1, m):
            send(squares.at[a], squares_in.at[a, col], square_send, square_recv.at[a], {"cols": lax.rem(col + d, m)})

    def send_spread(a, half, d_second):
        n_first, n_second = extents(half)
        slab = piece(a, copies[a], spot(half, 0, n_second - d_second), half)
        for d_first in range(1, n_first):
            send(slab, slab, send_sem.at[a], spread_recv.at[a], {"batch": spot(half, d_first, 0)})

    def update(a):
        drain(squares_in.at[a, pl.ds(0, m - 1)], square_recv.at[a])
        both = squares_in[a, 0]
        for d in range(1, m):
            both = both + squares_in[a, d]
        ratio = learn_rate * (jnp.sqrt(both[0:1]) * lax.rsqrt(both[1:2] + 1e-06))
        rows, columns = total[a].shape
        if a < 3:
            ratio = jnp.broadcast_to(ratio, (LANES, rows)).T
            for start in range(0, columns, LANES):
                block = slice(start, start + LANES)
                news[a][:, block] = own_weight[a][:, block] - total[a][:, block] * ratio
        else:
            news[a][...] = own_weight[a][...] - total[a][...] * ratio
        depth = rows // 2
        for half in range(2):
            piece(a, copies[a], me, half)[...] = news[a][half * depth : (half + 1) * depth].astype(jnp.bfloat16)
        for half in range(2):
            slab = piece(a, copies[a], me, half)
            for d_second in range(1, extents(half)[1]):
                send(slab, slab, send_sem.at[a], back_recv.at[a], {"batch": spot(half, 0, d_second)})
        for half in range(2):
            send_spread(a, half, 0)

    def pass_on(a):
        drain(used_second(a, second_in), back_recv.at[a])
        for half in range(2):
            for d_second in range(1, extents(half)[1]):
                send_spread(a, half, d_second)

    def update_small():
        drain(small_in.at[pl.ds(0, n - 1)], small_sem.at[1])
        for k in range(n):
            value = small_in[0, k]
            for j in range(1, n):
                value = value + small_in[j, k]
            small_done[share, k] = small_in[k, n] - learn_rate * (value * rate)
        for d in range(1, shares):
            to = {"cols": col - share + lax.rem(share + d, shares)}
            send(small_done.at[share], small_done.at[share], done_sem.at[0], done_sem.at[1], to)

    def gather_small():
        drain(small_done.at[pl.ds(0, shares - 1)], done_sem.at[1])
        for i in range(2):
            for k in range(n):
                for j in range(per_array):
                    small_full[i, k, :, j * chunk : (j + 1) * chunk] = small_done[i * per_array + j, k]
            small_own[i] = small_full[i, me]

    steps = dict(
        F=send_first, S=send_small, W=weigh, A=add_first, B=add_second, U=update, P=pass_on
    )
    steps.update(N=update_small, M=gather_small, E=enter_row)
    for step in ORDER:
        steps[step[0]](*map(int, step[1:]))
    drain(small_in.at[pl.ds(0, n - 1)], small_sem.at[0])
    drain(small_done.at[pl.ds(0, shares - 1)], done_sem.at[0])
    drain(squares_in.at[:, pl.ds(0, m - 1)], square_send)
    for a in range(4):
        drain(unit_out[a], unit_send.at[a])
    for a in range(4):
        rows, columns = full[a].shape
        slabs = 2 * sum((extents(h)[0] - 1) * extents(h)[1] + extents(h)[1] - 1 for h in range(2))
        sent = slabs * (total[a].shape[0] // 2) * total[a].shape[1] // 2
        drain(full[a].at[pl.ds(0, sent // columns)], send_sem.at[a])
        drain_first(a, first_in, spread_recv.at[a])


def finish(n, *refs):
    results, full, own = refs[0:8], refs[8], refs[9]
    outs, small_copies, small_news = refs[10:18], refs[18:20], refs[20:22]
    copy_rows, new_rows, sem, small_sem = refs[22:24], refs[24:26], refs[26], refs[27]
    moves = [pltpu.make_async_copy(results[i], outs[i], sem.at[i]) for i in range(8)]
    for move in moves:
        move.start()
    width = full.shape[-1]
    for i in range(2):
        for j in range(n):
            copy_rows[i][j * width : (j + 1) * width] = full[i, j, 0].astype(jnp.bfloat16)
        new_rows[i][...] = own[i, 0]
    for i in range(2):
        moves.append(pltpu.make_async_copy(copy_rows[i], small_copies[i], small_sem.at[i]))
        moves.append(pltpu.make_async_copy(new_rows[i], small_news[i], small_sem.at[2 + i]))
    for move in moves[8:]:
        move.start()
    for move in moves:
        move.wait()


def solution(mesh):
    n, m = mesh.shape["batch"], mesh.shape["cols"]
    n_x = math.isqrt(n)
    if n_x * n_x != n:
        n_x = n
    n_y = n // n_x
    most = max(n_x, n_y)

    def per_device(*args):
        args = args[:10] + tuple(w.reshape(1, -1) for w in args[10:])
        grads, weights, width = args[0:4], args[6:10], args[10].shape[1]
        blocks = [w.shape for w in weights]
        slices = blocks[0][0]
        slabs = [(b[0] // 2, b[1]) for b in blocks]
        lines = [(1, s[0]) for s in slabs[:3]] + [(1, slabs[3][1])]
        f32, bf16 = jnp.float32, jnp.bfloat16
        DMA = pltpu.SemaphoreType.DMA
        hops = max(most - 1, 1)
        pieces = math.gcd(max(width // LANES, 1), m // 2)
        hbm = pl.BlockSpec(memory_space=pltpu.HBM)
        vmem = pl.BlockSpec(memory_space=pltpu.VMEM)
        out_shape = (
            [jax.ShapeDtypeStruct(g.shape[1:], bf16) for g in grads]
            + [jax.ShapeDtypeStruct(b, f32) for b in blocks]
            + [jax.ShapeDtypeStruct((2, n, 1, width), f32), jax.ShapeDtypeStruct((2, 1, width), f32)]
        )
        results = pl.pallas_call(
            functools.partial(kernel, n, m, n_x, n_y),
            out_shape=[pltpu.VMEM(o.shape, o.dtype) for o in out_shape],
            in_specs=[hbm] * 12,
            out_specs=[vmem] * 10,
            scratch_shapes=(
                [pltpu.VMEM(g.shape[1:], f32) for g in grads]
                + [pltpu.VMEM(b, f32) for b in blocks] * 2
                + [pltpu.VMEM((2, hops, most) + s, bf16) for s in slabs] * 2
                + [pltpu.VMEM((2, hops) + s, bf16) for s in slabs] * 2
                + [pltpu.VMEM((2, hops, most + 1) + l, f32) for l in lines]
                + [pltpu.VMEM((2, hops, most) + l, f32) for l in lines]
                + [pltpu.VMEM((2, hops) + l, f32) for l in lines]
                + [
                    pltpu.VMEM((4, 2, slices), f32),
                    pltpu.VMEM((4, m, 2, slices), f32),
                    pltpu.VMEM((2, 1, (n + 1) * width), f32),
                    pltpu.VMEM((n, n + 1, 1, width // pieces), f32),
                    pltpu.VMEM((2 * pieces, n, 1, width // pieces), f32),
                    DMA((2, hops)),
                    DMA((4,)),
                    DMA((4,)),
                    DMA,
                ]
                + [DMA((4,))] * 6
                + [DMA, DMA((4,)), DMA((4,)), DMA((4,)), DMA((2,)), DMA((2,))]
                + [pltpu.SemaphoreType.REGULAR] * 2
            ),
            compiler_params=pltpu.CompilerParams(
                collective_id=0, has_side_effects=True, vmem_limit_bytes=40 * 2**20
            ),
        )(*[pltpu.with_memory_space_constraint(v, pltpu.HBM) for v in args])
        done = pl.pallas_call(
            functools.partial(finish, n),
            out_shape=out_shape[:8]
            + [jax.ShapeDtypeStruct((n * width,), bf16)] * 2
            + [jax.ShapeDtypeStruct((width,), f32)] * 2,
            in_specs=[vmem] * 10,
            out_specs=[hbm] * 12,
            scratch_shapes=[pltpu.VMEM((n * width,), bf16)] * 2
            + [pltpu.VMEM((width,), f32)] * 2
            + [DMA((8,)), DMA((4,))],
            compiler_params=pltpu.CompilerParams(vmem_limit_bytes=2**20),
        )(*results)
        return tuple(done[0:4]) + tuple(done[8:10]) + tuple(done[4:8]) + tuple(done[10:12])

    in_specs = (
        (P("batch", None, "cols"),) * 3
        + (P("batch", "cols", None),)
        + (P("batch", None),) * 2
        + (P("batch", "cols"),) * 3
        + (P("cols", "batch"),)
        + (P("batch"),) * 2
    )
    out_specs = (
        (P(None, "cols"),) * 3
        + (P("cols", None),)
        + (P(),) * 2
        + (P("batch", "cols"),) * 3
        + (P("cols", "batch"),)
        + (P("batch"),) * 2
    )
    return jax.shard_map(per_device, mesh=mesh, in_specs=in_specs, out_specs=out_specs, check_vma=False)
```

```python
import functools
import math

import jax
import jax.numpy as jnp
from jax import lax
from jax.experimental import pallas as pl
from jax.experimental.pallas import tpu as pltpu
from jax.sharding import PartitionSpec as P

learn_rate = 0.4
LANES = 128
LOW, SPAN, TINY = 87.0, 175.0, 1e-30
TURNED = 2
ORDER = (
    ('F0', 'F1', 'W0', 'W1', 'W2', 'W3', 'A0', 'S', 'F2', 'A1', 'F3', 'G2', 'E', 'N', 'B0', 'B1', 'U0', 'A2', 'A3', 'B2', 'U1', 'P0', 'M', 'B3', 'U2', 'P1', 'U3', 'P2', 'P3')
)


def across(a, line, depth):
    return jnp.broadcast_to(line, (LANES, depth)).T if a < 3 else line


def blocks_of(a, columns):
    step = LANES if a < 3 else columns
    return [slice(start, start + step) for start in range(0, columns, step)]


def encode(a, value, code, unit):
    depth, columns = value.shape
    size = jnp.abs(value)
    if a < 3:
        size = functools.reduce(jnp.maximum, [size[:, block] for block in blocks_of(a, columns)]).T
    largest = jnp.maximum(jnp.max(size, axis=0, keepdims=True), TINY)
    unit[...] = largest * SPAN**-2
    gain = across(a, SPAN**2 / largest, depth)
    for block in blocks_of(a, columns):
        part = value[:, block]
        level = jnp.abs(part) * gain
        level = jnp.exp(level * lax.rsqrt(level + TINY) - LOW)
        code[:, block] = jnp.where(part < 0, -level, level).astype(jnp.bfloat16)


def decode(a, code, unit):
    rows, columns = code.shape
    scale = across(a, unit[...], unit.shape[1])[:rows]
    parts = []
    for block in blocks_of(a, columns):
        part = code[:, block].astype(jnp.float32)
        root = jnp.log(jnp.abs(part)) + LOW
        level = root * root * scale
        parts.append(jnp.where(part < 0, -level, level))
    return jnp.concatenate(parts, axis=1) if len(parts) > 1 else parts[0]


def drain(ref, sem):
    pltpu.make_async_copy(ref, ref, sem).wait()


def kernel(n, m, n_x, n_y, turned, *refs):
    grads, small_grads = refs[0:4], refs[4:6]
    weights, small_weights = refs[6:10], refs[10:12]
    copies, news = refs[12:16], refs[16:20]
    small_full, small_own = refs[20:22]
    scratch = refs[22:]
    full, total, own_weight = scratch[0:4], scratch[4:8], scratch[8:12]
    first_out, first_in = scratch[12:16], scratch[16:20]
    second_out, second_in = scratch[20:24], scratch[24:28]
    unit_out, first_unit, second_unit = scratch[28:32], scratch[32:36], scratch[36:40]
    squares, squares_in, small_hold, small_in, small_done = scratch[40:45]
    turned_in, turned_unit = scratch[45:47]
    (
        early_sem, load_sem, weight_sem, small_local,
        send_sem, unit_send,
        first_recv, first_unit_recv, second_recv, second_unit_recv,
        square_send, square_recv, back_recv, spread_recv,
        small_sem, done_sem, turned_sem, plane_sem, row_sem,
    ) = scratch[47:]
    rate = n ** (-0.5)
    most = max(n_x, n_y)

    me = lax.axis_index("batch")
    col = lax.axis_index("cols")
    y, x = me // n_x, lax.rem(me, n_x)

    def spot(half, d_first, d_second):
        if half == 0:
            return lax.rem(y + d_second, n_y) * n_x + lax.rem(x + d_first, n_x)
        return lax.rem(y + d_first, n_y) * n_x + lax.rem(x + d_second, n_x)

    def extents(half):
        return (n_x, n_y) if half == 0 else (n_y, n_x)

    def piece(a, ref, chunk, half):
        rows, columns = total[a].shape
        depth = rows // 2
        if a < 3:
            start = pl.multiple_of(chunk * rows + half * depth, depth)
            return ref.at[pl.ds(start, depth), :]
        start = pl.multiple_of(chunk * columns, columns)
        return ref.at[pl.ds(half * depth, depth), pl.ds(start, columns)]

    def slots(a, ref, half):
        n_first, n_second = extents(half)
        return ref[a].at[half, pl.ds(0, n_first - 1), pl.ds(0, n_second)]

    odd = lax.rem(col, 2)
    row_col = col - odd
    plane_col = row_col + 1
    barrier = pltpu.get_barrier_semaphore()

    def greet(skip, **device):
        @pl.when(jnp.logical_not(skip))
        def _():
            pl.semaphore_signal(barrier, inc=1, device_id=device)

    neighbours = [spot(0, d, 0) for d in range(1, n_x)] + [spot(0, 0, d) for d in range(1, n_y)]
    for other in neighbours:
        pl.semaphore_signal(barrier, inc=1, device_id={"batch": other, "cols": plane_col})
    greet(odd == 1, batch=me, cols=plane_col)
    for d in range(0, m, 2):
        other = lax.rem(row_col + d, m)
        greet(other == col, batch=me, cols=other)

    def enter_plane():
        @pl.when(odd == 1)
        def _():
            pl.semaphore_wait(barrier, 2 * len(neighbours) + 1)
            pl.semaphore_signal(plane_sem, inc=1, device_id={"cols": row_col})

        @pl.when(odd == 0)
        def _():
            pl.semaphore_wait(plane_sem, 1)

    def enter_row():
        @pl.when(odd == 0)
        def _():
            pl.semaphore_wait(barrier, m - 1)
            pl.semaphore_signal(row_sem, inc=1, device_id={"cols": plane_col})

        @pl.when(odd == 1)
        def _():
            pl.semaphore_wait(row_sem, 1)

    early, rest = {}, []
    for half in range(2):
        n_first, n_second = extents(half)
        for d_first in range(n_first):
            for d_second in range(n_second):
                here = spot(half, d_first, d_second)
                first_sent = d_first > 0 and d_second == n_second - 1
                copy = pltpu.make_async_copy(
                    piece(0, grads[0].at[0], here, half),
                    piece(0, full[0], here, half),
                    early_sem.at[half, d_first - 1] if first_sent else load_sem.at[0],
                )
                if first_sent:
                    early[half, d_first] = copy
                else:
                    rest.append(copy)
    width = small_weights[0].shape[1]
    shares, chunk = small_done.shape[0], small_done.shape[3]
    per_array = shares // 2
    share = lax.rem(col, shares)
    smalls, weight_loads = [], []
    for i in range(2):
        smalls.append((small_grads[i], small_hold.at[i, :, pl.ds(0, n * width)]))
        smalls.append((small_weights[i], small_hold.at[i, :, pl.ds(n * width, width)]))
    for copy in early.values():
        copy.start()
    for copy in rest:
        copy.start()
    for a in range(1, 4):
        pltpu.make_async_copy(grads[a].at[0], full[a], load_sem.at[a]).start()
        if a == 1:
            for b in range(4):
                weight_loads.append(pltpu.make_async_copy(weights[b], own_weight[b], weight_sem.at[b]))
                weight_loads[b].start()
            for source, target in smalls:
                pltpu.make_async_copy(source, target, small_local).start()

    def load_rest(a):
        if a == 0:
            drain(full[0].at[pl.ds(0, len(rest) * (total[0].shape[0] // 2))], load_sem.at[0])
        else:
            drain(full[a], load_sem.at[a])

    entered, loaded, ready = [], set(), []

    def send(source, target, sem, arrival, device):
        pltpu.make_async_remote_copy(
            src_ref=source, dst_ref=target, send_sem=sem, recv_sem=arrival, device_id=device
        ).start()

    def send_turned(half):
        a, at, top = TURNED, (half, 0, 1), pl.ds(0, turned)
        turns = me == (1 if half == 0 else 2)
        std = {"batch": spot(half, 1, 0)}
        code = first_out[a].at[at + (top,)]
        below = pl.ds(turned, total[a].shape[0] // 2 - turned)
        send(first_out[a].at[at + (below,)], first_in[a].at[at + (below,)], send_sem.at[a], first_recv.at[a], std)

        @pl.when(jnp.logical_not(turns))
        def _():
            send(code, first_in[a].at[at + (top,)], send_sem.at[a], first_recv.at[a], std)

        @pl.when(turns)
        def _():
            far = {"batch": n - 1}
            send(unit_out[a].at[at], turned_unit.at[half], turned_sem.at[0], turned_sem.at[1], far)
            send(code, turned_in.at[half], send_sem.at[a], turned_sem.at[2], far)

    def add_turned(a):
        if a not in loaded:
            loaded.add(a)
            load_rest(a)
        if turned and a == TURNED:
            @pl.when(me == n - 1)
            def _():
                drain(turned_unit, turned_sem.at[1])
                drain(turned_in, turned_sem.at[2])
                for half in range(2):
                    own = piece(a, full[a], spot(half, 1, 0), half).at[pl.ds(0, turned)]
                    own[...] = own[...] + decode(a, turned_in.at[half], turned_unit.at[half])

        send_first(a, [0])

    def send_first(a, ds=None):
        if ds is None:
            ds = range(most - 1, -1 if a != TURNED else 0, -1)
        for d in ds:
            for half in range(2):
                n_first, n_second = extents(half)
                for d_first in range(1, n_first):
                    if d >= n_second:
                        continue
                    if a == 0 and d == n_second - 1:
                        early[half, d_first].wait()
                    elif a not in loaded:
                        loaded.add(a)
                        load_rest(a)
                    at = (half, d_first - 1, d)
                    unit = unit_out[a].at[at]
                    encode(a, piece(a, full[a], spot(half, d_first, d), half)[...], first_out[a].at[at], unit)
                    to = {"batch": spot(half, d_first, 0)}
                    ready.append((unit, first_unit[a].at[at], unit_send.at[a], first_unit_recv.at[a], to))
                    if turned and a == TURNED and d == 1:
                        ready.append((half,))
                    else:
                        ready.append((first_out[a].at[at], first_in[a].at[at], send_sem.at[a], first_recv.at[a], to))
            if not entered:
                entered.append(True)
                enter_plane()
            for item in ready:
                send_turned(*item) if len(item) == 1 else send(*item)
            ready.clear()

    def send_small():
        drain(small_hold, small_local)
        start = lax.rem(share, per_array) * chunk
        for k in range(n + 1):
            small_in[me, k] = small_hold[share // per_array, :, pl.ds(pl.multiple_of(k * width + start, chunk), chunk)]
        for d in range(1, n):
            send(small_in.at[me], small_in.at[me], small_sem.at[0], small_sem.at[1], {"batch": lax.rem(me + d, n)})

    def row_squares(a, value):
        value = value * value
        if a == 3:
            return jnp.sum(value, axis=0, keepdims=True)
        folded = value[:, :LANES]
        for start in range(LANES, value.shape[1], LANES):
            folded = folded + value[:, start : start + LANES]
        return jnp.sum(folded.T, axis=0, keepdims=True)

    def weigh(a):
        weight_loads[a].wait()
        squares[a, 0:1] = row_squares(a, own_weight[a][...])

    def drain_first(a, ref, sem):
        if n_x == n_y:
            drain(ref[a], sem)
        else:
            for half in range(2):
                if extents(half)[0] > 1:
                    drain(slots(a, ref, half), sem)

    def add_first(a):
        if a not in loaded:
            loaded.add(a)
            load_rest(a)
        drain_first(a, first_unit, first_unit_recv.at[a])
        if turned and a == TURNED:
            @pl.when(me == 0)
            def _():
                drain(full[a].at[pl.ds(0, total[a].shape[0] - turned)], first_recv.at[a])

            @pl.when(me != 0)
            def _():
                drain_first(a, first_in, first_recv.at[a])
        else:
            drain_first(a, first_in, first_recv.at[a])
        for d_second in range(most - 1, -1, -1):
            for half in range(2):
                n_first, n_second = extents(half)
                if d_second >= n_second:
                    continue
                own = piece(a, full[a], spot(half, 0, d_second), half)
                value = own[...]
                for d_first in range(1, n_first):
                    at = (half, d_first - 1, d_second)
                    before, value = value, value + decode(a, first_in[a].at[at], first_unit[a].at[at])
                    if turned and a == TURNED and d_second == 1:
                        top = jnp.where(me == 0, before[:turned], value[:turned])
                        value = jnp.concatenate([top, value[turned:]], axis=0)
                if d_second == 0:
                    own[...] = value
                    continue
                at = (half, d_second - 1)
                unit = unit_out[a].at[at + (most,)]
                encode(a, value, second_out[a].at[at], unit)
                to = {"batch": spot(half, 0, d_second)}
                send(unit, second_unit[a].at[at], unit_send.at[a], second_unit_recv.at[a], to)
                send(second_out[a].at[at], second_in[a].at[at], send_sem.at[a], second_recv.at[a], to)

    def used_second(a, ref):
        if n_x == n_y:
            return ref[a]
        half = 0 if n_y > 1 else 1
        return ref[a].at[half, pl.ds(0, extents(half)[1] - 1)]

    def add_second(a):
        drain(used_second(a, second_unit), second_unit_recv.at[a])
        drain(used_second(a, second_in), second_recv.at[a])
        depth = total[a].shape[0] // 2
        for half in range(2):
            value = piece(a, full[a], me, half)[...]
            for d_second in range(1, extents(half)[1]):
                at = (half, d_second - 1)
                value = value + decode(a, second_in[a].at[at], second_unit[a].at[at])
            total[a][half * depth : (half + 1) * depth] = value * rate
        squares[a, 1:2] = row_squares(a, total[a][...])
        squares_in[a, col] = squares[a]
        for d in range(1, m):
            send(squares.at[a], squares_in.at[a, col], square_send, square_recv.at[a], {"cols": lax.rem(col + d, m)})

    def send_spread(a, half, d_second):
        n_first, n_second = extents(half)
        slab = piece(a, copies[a], spot(half, 0, n_second - d_second), half)
        for d_first in range(1, n_first):
            send(slab, slab, send_sem.at[a], spread_recv.at[a], {"batch": spot(half, d_first, 0)})

    def update(a):
        drain(squares_in.at[a, pl.ds(0, m - 1)], square_recv.at[a])
        both = squares_in[a, 0]
        for d in range(1, m):
            both = both + squares_in[a, d]
        ratio = learn_rate * (jnp.sqrt(both[0:1]) * lax.rsqrt(both[1:2] + 1e-06))
        rows, columns = total[a].shape
        if a < 3:
            ratio = jnp.broadcast_to(ratio, (LANES, rows)).T
            for start in range(0, columns, LANES):
                block = slice(start, start + LANES)
                news[a][:, block] = own_weight[a][:, block] - total[a][:, block] * ratio
        else:
            news[a][...] = own_weight[a][...] - total[a][...] * ratio
        depth = rows // 2
        for half in range(2):
            piece(a, copies[a], me, half)[...] = news[a][half * depth : (half + 1) * depth].astype(jnp.bfloat16)
        for half in range(2):
            slab = piece(a, copies[a], me, half)
            for d_second in range(1, extents(half)[1]):
                send(slab, slab, send_sem.at[a], back_recv.at[a], {"batch": spot(half, 0, d_second)})
        for half in range(2):
            send_spread(a, half, 0)

    def pass_on(a):
        drain(used_second(a, second_in), back_recv.at[a])
        for half in range(2):
            for d_second in range(1, extents(half)[1]):
                send_spread(a, half, d_second)

    def update_small():
        drain(small_in.at[pl.ds(0, n - 1)], small_sem.at[1])
        for k in range(n):
            value = small_in[0, k]
            for j in range(1, n):
                value = value + small_in[j, k]
            small_done[share, k] = small_in[k, n] - learn_rate * (value * rate)
        for d in range(1, shares):
            to = {"cols": col - share + lax.rem(share + d, shares)}
            send(small_done.at[share], small_done.at[share], done_sem.at[0], done_sem.at[1], to)

    def gather_small():
        drain(small_done.at[pl.ds(0, shares - 1)], done_sem.at[1])
        for i in range(2):
            for k in range(n):
                for j in range(per_array):
                    small_full[i, k, :, j * chunk : (j + 1) * chunk] = small_done[i * per_array + j, k]
            small_own[i] = small_full[i, me]

    steps = dict(
        F=send_first, G=add_turned, S=send_small, W=weigh, A=add_first, B=add_second, U=update, P=pass_on
    )
    steps.update(N=update_small, M=gather_small, E=enter_row)
    for step in ORDER:
        steps[step[0]](*map(int, step[1:]))
    drain(small_in.at[pl.ds(0, n - 1)], small_sem.at[0])
    drain(small_done.at[pl.ds(0, shares - 1)], done_sem.at[0])
    drain(squares_in.at[:, pl.ds(0, m - 1)], square_send)
    for a in range(4):
        drain(unit_out[a], unit_send.at[a])
    if turned:
        @pl.when(jnp.logical_or(me == 1, me == 2))
        def _():
            drain(turned_unit.at[0], turned_sem.at[0])
    for a in range(4):
        rows, columns = full[a].shape
        slabs = 2 * sum((extents(h)[0] - 1) * extents(h)[1] + extents(h)[1] - 1 for h in range(2))
        sent = slabs * (total[a].shape[0] // 2) * total[a].shape[1] // 2
        drain(full[a].at[pl.ds(0, sent // columns)], send_sem.at[a])
        drain_first(a, first_in, spread_recv.at[a])


def finish(n, *refs):
    results, full, own = refs[0:8], refs[8], refs[9]
    outs, small_copies, small_news = refs[10:18], refs[18:20], refs[20:22]
    copy_rows, new_rows, sem, small_sem = refs[22:24], refs[24:26], refs[26], refs[27]
    moves = [pltpu.make_async_copy(results[i], outs[i], sem.at[i]) for i in range(8)]
    for move in moves:
        move.start()
    width = full.shape[-1]
    for i in range(2):
        for j in range(n):
            copy_rows[i][j * width : (j + 1) * width] = full[i, j, 0].astype(jnp.bfloat16)
        new_rows[i][...] = own[i, 0]
    for i in range(2):
        moves.append(pltpu.make_async_copy(copy_rows[i], small_copies[i], small_sem.at[i]))
        moves.append(pltpu.make_async_copy(new_rows[i], small_news[i], small_sem.at[2 + i]))
    for move in moves[8:]:
        move.start()
    for move in moves:
        move.wait()


def solution(mesh):
    n, m = mesh.shape["batch"], mesh.shape["cols"]
    n_x = math.isqrt(n)
    if n_x * n_x != n:
        n_x = n
    n_y = n // n_x
    most = max(n_x, n_y)

    def per_device(*args):
        args = args[:10] + tuple(w.reshape(1, -1) for w in args[10:])
        grads, weights, width = args[0:4], args[6:10], args[10].shape[1]
        blocks = [w.shape for w in weights]
        slices = blocks[0][0]
        slabs = [(b[0] // 2, b[1]) for b in blocks]
        lines = [(1, s[0]) for s in slabs[:3]] + [(1, slabs[3][1])]
        f32, bf16 = jnp.float32, jnp.bfloat16
        DMA = pltpu.SemaphoreType.DMA
        hops = max(most - 1, 1)
        turned = slabs[TURNED][0] * 6 // 256 * 16 if n_x == n_y == 2 else 0
        pieces = math.gcd(max(width // LANES, 1), m // 2)
        hbm = pl.BlockSpec(memory_space=pltpu.HBM)
        vmem = pl.BlockSpec(memory_space=pltpu.VMEM)
        out_shape = (
            [jax.ShapeDtypeStruct(g.shape[1:], bf16) for g in grads]
            + [jax.ShapeDtypeStruct(b, f32) for b in blocks]
            + [jax.ShapeDtypeStruct((2, n, 1, width), f32), jax.ShapeDtypeStruct((2, 1, width), f32)]
        )
        results = pl.pallas_call(
            functools.partial(kernel, n, m, n_x, n_y, turned),
            out_shape=[pltpu.VMEM(o.shape, o.dtype) for o in out_shape],
            in_specs=[hbm] * 12,
            out_specs=[vmem] * 10,
            scratch_shapes=(
                [pltpu.VMEM(g.shape[1:], f32) for g in grads]
                + [pltpu.VMEM(b, f32) for b in blocks] * 2
                + [pltpu.VMEM((2, hops, most) + s, bf16) for s in slabs] * 2
                + [pltpu.VMEM((2, hops) + s, bf16) for s in slabs] * 2
                + [pltpu.VMEM((2, hops, most + 1) + l, f32) for l in lines]
                + [pltpu.VMEM((2, hops, most) + l, f32) for l in lines]
                + [pltpu.VMEM((2, hops) + l, f32) for l in lines]
                + [
                    pltpu.VMEM((4, 2, slices), f32),
                    pltpu.VMEM((4, m, 2, slices), f32),
                    pltpu.VMEM((2, 1, (n + 1) * width), f32),
                    pltpu.VMEM((n, n + 1, 1, width // pieces), f32),
                    pltpu.VMEM((2 * pieces, n, 1, width // pieces), f32),
                    pltpu.VMEM((2, max(turned, 16)) + slabs[TURNED][1:], bf16),
                    pltpu.VMEM((2,) + lines[TURNED], f32),
                    DMA((2, hops)),
                    DMA((4,)),
                    DMA((4,)),
                    DMA,
                ]
                + [DMA((4,))] * 6
                + [DMA, DMA((4,)), DMA((4,)), DMA((4,)), DMA((2,)), DMA((2,)), DMA((3,))]
                + [pltpu.SemaphoreType.REGULAR] * 2
            ),
            compiler_params=pltpu.CompilerParams(
                collective_id=0, has_side_effects=True, vmem_limit_bytes=40 * 2**20
            ),
        )(*[pltpu.with_memory_space_constraint(v, pltpu.HBM) for v in args])
        done = pl.pallas_call(
            functools.partial(finish, n),
            out_shape=out_shape[:8]
            + [jax.ShapeDtypeStruct((n * width,), bf16)] * 2
            + [jax.ShapeDtypeStruct((width,), f32)] * 2,
            in_specs=[vmem] * 10,
            out_specs=[hbm] * 12,
            scratch_shapes=[pltpu.VMEM((n * width,), bf16)] * 2
            + [pltpu.VMEM((width,), f32)] * 2
            + [DMA((8,)), DMA((4,))],
            compiler_params=pltpu.CompilerParams(vmem_limit_bytes=2**20),
        )(*results)
        return tuple(done[0:4]) + tuple(done[8:10]) + tuple(done[4:8]) + tuple(done[10:12])

    in_specs = (
        (P("batch", None, "cols"),) * 3
        + (P("batch", "cols", None),)
        + (P("batch", None),) * 2
        + (P("batch", "cols"),) * 3
        + (P("cols", "batch"),)
        + (P("batch"),) * 2
    )
    out_specs = (
        (P(None, "cols"),) * 3
        + (P("cols", None),)
        + (P(),) * 2
        + (P("batch", "cols"),) * 3
        + (P("cols", "batch"),)
        + (P("batch"),) * 2
    )
    return jax.shard_map(per_device, mesh=mesh, in_specs=in_specs, out_specs=out_specs, check_vma=False)
```

```python
import functools
import math

import jax
import jax.numpy as jnp
from jax import lax
from jax.experimental import pallas as pl
from jax.experimental.pallas import tpu as pltpu
from jax.sharding import PartitionSpec as P

learn_rate = 0.4
LANES = 128
LOW, SPAN, TINY = 87.0, 175.0, 1e-30
TURNED = 2
ORDER = (
    ('F0', 'F1', 'F2', 'W0', 'W1', 'W2', 'W3', 'A0', 'S', 'A1', 'G2', 'F3', 'E', 'N', 'B0', 'B1', 'A2', 'U0', 'A3', 'U1', 'B2', 'B3', 'P0', 'M', 'U2', 'U3', 'P1', 'P2', 'P3')
)


def across(a, line, depth):
    return jnp.broadcast_to(line, (LANES, depth)).T if a < 3 else line


def blocks_of(a, columns):
    step = LANES if a < 3 else columns
    return [slice(start, start + step) for start in range(0, columns, step)]


def encode(a, value, code, unit):
    depth, columns = value.shape
    size = jnp.abs(value)
    if a < 3:
        size = functools.reduce(jnp.maximum, [size[:, block] for block in blocks_of(a, columns)]).T
    largest = jnp.maximum(jnp.max(size, axis=0, keepdims=True), TINY)
    unit[...] = largest * SPAN**-2
    gain = across(a, SPAN**2 / largest, depth)
    for block in blocks_of(a, columns):
        part = value[:, block]
        level = jnp.abs(part) * gain
        level = jnp.exp(level * lax.rsqrt(level + TINY) - LOW)
        code[:, block] = jnp.where(part < 0, -level, level).astype(jnp.bfloat16)


def decode(a, code, unit):
    rows, columns = code.shape
    scale = across(a, unit[...], unit.shape[1])[:rows]
    parts = []
    for block in blocks_of(a, columns):
        part = code[:, block].astype(jnp.float32)
        root = jnp.log(jnp.abs(part)) + LOW
        level = root * root * scale
        parts.append(jnp.where(part < 0, -level, level))
    return jnp.concatenate(parts, axis=1) if len(parts) > 1 else parts[0]


def drain(ref, sem):
    pltpu.make_async_copy(ref, ref, sem).wait()


def kernel(n, m, n_x, n_y, turned, *refs):
    grads, small_grads = refs[0:4], refs[4:6]
    weights, small_weights = refs[6:10], refs[10:12]
    copies, news = refs[12:16], refs[16:20]
    small_full, small_own = refs[20:22]
    scratch = refs[22:]
    full, total, own_weight = scratch[0:4], scratch[4:8], scratch[8:12]
    first_out, first_in = scratch[12:16], scratch[16:20]
    second_out, second_in = scratch[20:24], scratch[24:28]
    unit_out, first_unit, second_unit = scratch[28:32], scratch[32:36], scratch[36:40]
    squares, squares_in, small_hold, small_in, small_done = scratch[40:45]
    turned_in, turned_unit = scratch[45:47]
    (
        early_sem, load_sem, weight_sem, small_local,
        unit_send,
        first_recv, first_unit_recv, second_recv, second_unit_recv,
        square_send, square_recv,
        small_arrived, done_sem, turned_sem, plane_sem, row_sem,
    ) = scratch[47:]
    sent = (early_sem,) + tuple(load_sem.at[a] for a in range(1, 4))
    back_recv, spread_recv = first_unit_recv, first_recv
    rate = n ** (-0.5)
    most = max(n_x, n_y)

    me = lax.axis_index("batch")
    col = lax.axis_index("cols")
    y, x = me // n_x, lax.rem(me, n_x)

    def spot(half, d_first, d_second):
        if half == 0:
            return lax.rem(y + d_second, n_y) * n_x + lax.rem(x + d_first, n_x)
        return lax.rem(y + d_first, n_y) * n_x + lax.rem(x + d_second, n_x)

    def extents(half):
        return (n_x, n_y) if half == 0 else (n_y, n_x)

    def piece(a, ref, chunk, half):
        rows, columns = total[a].shape
        depth = rows // 2
        if a < 3:
            start = pl.multiple_of(chunk * rows + half * depth, depth)
            return ref.at[pl.ds(start, depth), :]
        start = pl.multiple_of(chunk * columns, columns)
        return ref.at[pl.ds(half * depth, depth), pl.ds(start, columns)]

    def slots(a, ref, half):
        n_first, n_second = extents(half)
        return ref[a].at[half, pl.ds(0, n_first - 1), pl.ds(0, n_second)]

    odd = lax.rem(col, 2)
    row_col = col - odd
    plane_col = row_col + 1
    barrier = pltpu.get_barrier_semaphore()

    def greet(skip, **device):
        @pl.when(jnp.logical_not(skip))
        def _():
            pl.semaphore_signal(barrier, inc=1, device_id=device)

    neighbours = [spot(0, d, 0) for d in range(1, n_x)] + [spot(0, 0, d) for d in range(1, n_y)]
    for other in neighbours:
        pl.semaphore_signal(barrier, inc=1, device_id={"batch": other, "cols": plane_col})
    greet(odd == 1, batch=me, cols=plane_col)
    for d in range(0, m, 2):
        other = lax.rem(row_col + d, m)
        greet(other == col, batch=me, cols=other)

    def enter_plane():
        @pl.when(odd == 1)
        def _():
            pl.semaphore_wait(barrier, 2 * len(neighbours) + 1)
            pl.semaphore_signal(plane_sem, inc=1, device_id={"cols": row_col})

        @pl.when(odd == 0)
        def _():
            pl.semaphore_wait(plane_sem, 1)

    def enter_row():
        @pl.when(odd == 0)
        def _():
            pl.semaphore_wait(barrier, m - 1)
            pl.semaphore_signal(row_sem, inc=1, device_id={"cols": plane_col})

        @pl.when(odd == 1)
        def _():
            pl.semaphore_wait(row_sem, 1)

    early, rest = {}, []
    for half in range(2):
        n_first, n_second = extents(half)
        for d_first in range(n_first):
            for d_second in range(n_second):
                here = spot(half, d_first, d_second)
                first_sent = d_first > 0 and d_second == n_second - 1
                copy = pltpu.make_async_copy(
                    piece(0, grads[0].at[0], here, half),
                    piece(0, full[0], here, half),
                    early_sem if first_sent else load_sem.at[0],
                )
                if first_sent:
                    early[half, d_first] = copy
                else:
                    rest.append(copy)
    width = small_weights[0].shape[1]
    shares, chunk = small_done.shape[0], small_done.shape[3]
    per_array = shares // 2
    share = lax.rem(col, shares)
    smalls, weight_loads = [], []
    for i in range(2):
        smalls.append((small_grads[i], small_hold.at[i, :, pl.ds(0, n * width)]))
        smalls.append((small_weights[i], small_hold.at[i, :, pl.ds(n * width, width)]))
    for copy in early.values():
        copy.start()
    for copy in rest:
        copy.start()
    for a in range(1, 4):
        pltpu.make_async_copy(grads[a].at[0], full[a], load_sem.at[a]).start()
        if a == 1:
            for b in range(4):
                weight_loads.append(pltpu.make_async_copy(weights[b], own_weight[b], weight_sem.at[b]))
                weight_loads[b].start()
            for source, target in smalls:
                pltpu.make_async_copy(source, target, small_local).start()

    def load_rest(a):
        if a == 0:
            drain(full[0].at[pl.ds(0, len(rest) * (total[0].shape[0] // 2))], load_sem.at[0])
        else:
            drain(full[a], load_sem.at[a])

    entered, loaded, ready = [], set(), []

    def send(source, target, sem, arrival, device):
        pltpu.make_async_remote_copy(
            src_ref=source, dst_ref=target, send_sem=sem, recv_sem=arrival, device_id=device
        ).start()

    def send_turned(half):
        a, at, top = TURNED, (half, 0, 1), pl.ds(0, turned)
        turns = me == (1 if half == 0 else 2)
        std = {"batch": spot(half, 1, 0)}
        code = first_out[a].at[at + (top,)]
        below = pl.ds(turned, total[a].shape[0] // 2 - turned)
        send(first_out[a].at[at + (below,)], first_in[a].at[at + (below,)], sent[a], first_recv.at[a], std)

        @pl.when(jnp.logical_not(turns))
        def _():
            send(code, first_in[a].at[at + (top,)], sent[a], first_recv.at[a], std)

        @pl.when(turns)
        def _():
            far = {"batch": n - 1}
            send(unit_out[a].at[at], turned_unit.at[half], turned_sem.at[0], turned_sem.at[1], far)
            send(code, turned_in.at[half], sent[a], turned_sem.at[2], far)

    def add_turned(a):
        if a not in loaded:
            loaded.add(a)
            load_rest(a)
        if turned and a == TURNED:
            @pl.when(me == n - 1)
            def _():
                drain(turned_unit, turned_sem.at[1])
                drain(turned_in, turned_sem.at[2])
                for half in range(2):
                    own = piece(a, full[a], spot(half, 1, 0), half).at[pl.ds(0, turned)]
                    own[...] = own[...] + decode(a, turned_in.at[half], turned_unit.at[half])

        send_first(a, [0])

    def send_first(a, ds=None):
        if ds is None:
            ds = range(most - 1, -1 if a != TURNED else 0, -1)
        for d in ds:
            for half in range(2):
                n_first, n_second = extents(half)
                for d_first in range(1, n_first):
                    if d >= n_second:
                        continue
                    if a == 0 and d == n_second - 1:
                        if early:
                            drain(full[0].at[pl.ds(0, len(early) * (total[0].shape[0] // 2))], early_sem)
                            early.clear()
                    elif a not in loaded:
                        loaded.add(a)
                        load_rest(a)
                    at = (half, d_first - 1, d)
                    unit = unit_out[a].at[at]
                    encode(a, piece(a, full[a], spot(half, d_first, d), half)[...], first_out[a].at[at], unit)
                    to = {"batch": spot(half, d_first, 0)}
                    ready.append((unit, first_unit[a].at[at], unit_send.at[a], first_unit_recv.at[a], to))
                    if turned and a == TURNED and d == 1:
                        ready.append((half,))
                    else:
                        ready.append((first_out[a].at[at], first_in[a].at[at], sent[a], first_recv.at[a], to))
            if not entered:
                entered.append(True)
                enter_plane()
            for item in ready:
                send_turned(*item) if len(item) == 1 else send(*item)
            ready.clear()

    def send_small():
        drain(small_hold, small_local)
        start = lax.rem(share, per_array) * chunk
        for k in range(n + 1):
            small_in[me, k] = small_hold[share // per_array, :, pl.ds(pl.multiple_of(k * width + start, chunk), chunk)]
        for d in range(1, n):
            send(small_in.at[me], small_in.at[me], small_local, small_arrived, {"batch": lax.rem(me + d, n)})

    def row_squares(a, value):
        value = value * value
        if a == 3:
            return jnp.sum(value, axis=0, keepdims=True)
        folded = value[:, :LANES]
        for start in range(LANES, value.shape[1], LANES):
            folded = folded + value[:, start : start + LANES]
        return jnp.sum(folded.T, axis=0, keepdims=True)

    def weigh(a):
        weight_loads[a].wait()
        squares[a, 0:1] = row_squares(a, own_weight[a][...])

    def drain_first(a, ref, sem):
        if n_x == n_y:
            drain(ref[a], sem)
        else:
            for half in range(2):
                if extents(half)[0] > 1:
                    drain(slots(a, ref, half), sem)

    def add_first(a):
        if a not in loaded:
            loaded.add(a)
            load_rest(a)
        drain_first(a, first_unit, first_unit_recv.at[a])
        if turned and a == TURNED:
            @pl.when(me == 0)
            def _():
                drain(full[a].at[pl.ds(0, total[a].shape[0] - turned)], first_recv.at[a])

            @pl.when(me != 0)
            def _():
                drain_first(a, first_in, first_recv.at[a])
        else:
            drain_first(a, first_in, first_recv.at[a])
        for d_second in range(most - 1, -1, -1):
            for half in range(2):
                n_first, n_second = extents(half)
                if d_second >= n_second:
                    continue
                own = piece(a, full[a], spot(half, 0, d_second), half)
                value = own[...]
                for d_first in range(1, n_first):
                    at = (half, d_first - 1, d_second)
                    before, value = value, value + decode(a, first_in[a].at[at], first_unit[a].at[at])
                    if turned and a == TURNED and d_second == 1:
                        top = jnp.where(me == 0, before[:turned], value[:turned])
                        value = jnp.concatenate([top, value[turned:]], axis=0)
                if d_second == 0:
                    own[...] = value
                    continue
                at = (half, d_second - 1)
                unit = unit_out[a].at[at + (most,)]
                encode(a, value, second_out[a].at[at], unit)
                to = {"batch": spot(half, 0, d_second)}
                send(unit, second_unit[a].at[at], unit_send.at[a], second_unit_recv.at[a], to)
                send(second_out[a].at[at], second_in[a].at[at], sent[a], second_recv.at[a], to)

    def used_second(a, ref):
        if n_x == n_y:
            return ref[a]
        half = 0 if n_y > 1 else 1
        return ref[a].at[half, pl.ds(0, extents(half)[1] - 1)]

    def add_second(a):
        drain(used_second(a, second_unit), second_unit_recv.at[a])
        drain(used_second(a, second_in), second_recv.at[a])
        depth = total[a].shape[0] // 2
        for half in range(2):
            value = piece(a, full[a], me, half)[...]
            for d_second in range(1, extents(half)[1]):
                at = (half, d_second - 1)
                value = value + decode(a, second_in[a].at[at], second_unit[a].at[at])
            total[a][half * depth : (half + 1) * depth] = value * rate
        squares[a, 1:2] = row_squares(a, total[a][...])
        squares_in[a, col] = squares[a]
        for d in range(1, m):
            send(squares.at[a], squares_in.at[a, col], square_send, square_recv.at[a], {"cols": lax.rem(col + d, m)})

    def send_spread(a, half, d_second):
        n_first, n_second = extents(half)
        slab = piece(a, copies[a], spot(half, 0, n_second - d_second), half)
        for d_first in range(1, n_first):
            send(slab, slab, sent[a], spread_recv.at[a], {"batch": spot(half, d_first, 0)})

    def update(a):
        drain(squares_in.at[a, pl.ds(0, m - 1)], square_recv.at[a])
        both = squares_in[a, 0]
        for d in range(1, m):
            both = both + squares_in[a, d]
        ratio = learn_rate * (jnp.sqrt(both[0:1]) * lax.rsqrt(both[1:2] + 1e-06))
        rows, columns = total[a].shape
        if a < 3:
            ratio = jnp.broadcast_to(ratio, (LANES, rows)).T
            for start in range(0, columns, LANES):
                block = slice(start, start + LANES)
                news[a][:, block] = own_weight[a][:, block] - total[a][:, block] * ratio
        else:
            news[a][...] = own_weight[a][...] - total[a][...] * ratio
        depth = rows // 2
        for half in range(2):
            piece(a, copies[a], me, half)[...] = news[a][half * depth : (half + 1) * depth].astype(jnp.bfloat16)
        for half in range(2):
            slab = piece(a, copies[a], me, half)
            for d_second in range(1, extents(half)[1]):
                send(slab, slab, sent[a], back_recv.at[a], {"batch": spot(half, 0, d_second)})
        for half in range(2):
            send_spread(a, half, 0)

    def pass_on(a):
        drain(used_second(a, second_in), back_recv.at[a])
        for half in range(2):
            for d_second in range(1, extents(half)[1]):
                send_spread(a, half, d_second)

    def update_small():
        drain(small_in.at[pl.ds(0, n - 1)], small_arrived)
        for k in range(n):
            value = small_in[0, k]
            for j in range(1, n):
                value = value + small_in[j, k]
            small_done[share, k] = small_in[k, n] - learn_rate * (value * rate)
        for d in range(1, shares):
            to = {"cols": col - share + lax.rem(share + d, shares)}
            send(small_done.at[share], small_done.at[share], done_sem.at[0], done_sem.at[1], to)

    def gather_small():
        drain(small_done.at[pl.ds(0, shares - 1)], done_sem.at[1])
        for i in range(2):
            for k in range(n):
                for j in range(per_array):
                    small_full[i, k, :, j * chunk : (j + 1) * chunk] = small_done[i * per_array + j, k]
            small_own[i] = small_full[i, me]

    steps = dict(
        F=send_first, G=add_turned, S=send_small, W=weigh, A=add_first, B=add_second, U=update, P=pass_on
    )
    steps.update(N=update_small, M=gather_small, E=enter_row)
    for step in ORDER:
        steps[step[0]](*map(int, step[1:]))
    drain(small_in.at[pl.ds(0, n - 1)], small_local)
    drain(small_done.at[pl.ds(0, shares - 1)], done_sem.at[0])
    drain(squares_in.at[:, pl.ds(0, m - 1)], square_send)
    for a in range(4):
        drain(unit_out[a], unit_send.at[a])
    if turned:
        @pl.when(jnp.logical_or(me == 1, me == 2))
        def _():
            drain(turned_unit.at[0], turned_sem.at[0])
    for a in range(4):
        rows, columns = full[a].shape
        slabs = 2 * sum((extents(h)[0] - 1) * extents(h)[1] + extents(h)[1] - 1 for h in range(2))
        gone = slabs * (total[a].shape[0] // 2) * total[a].shape[1] // 2
        drain(full[a].at[pl.ds(0, gone // columns)], sent[a])
        drain_first(a, first_in, spread_recv.at[a])


def finish(n, *refs):
    results, full, own = refs[0:8], refs[8], refs[9]
    outs, small_copies, small_news = refs[10:18], refs[18:20], refs[20:22]
    copy_rows, new_rows, sem, small_sem = refs[22:24], refs[24:26], refs[26], refs[27]
    moves = [pltpu.make_async_copy(results[i], outs[i], sem.at[i]) for i in range(8)]
    for move in moves:
        move.start()
    width = full.shape[-1]
    for i in range(2):
        for j in range(n):
            copy_rows[i][j * width : (j + 1) * width] = full[i, j, 0].astype(jnp.bfloat16)
        new_rows[i][...] = own[i, 0]
    for i in range(2):
        moves.append(pltpu.make_async_copy(copy_rows[i], small_copies[i], small_sem.at[i]))
        moves.append(pltpu.make_async_copy(new_rows[i], small_news[i], small_sem.at[2 + i]))
    for move in moves[8:]:
        move.start()
    for move in moves:
        move.wait()


def solution(mesh):
    n, m = mesh.shape["batch"], mesh.shape["cols"]
    n_x = math.isqrt(n)
    if n_x * n_x != n:
        n_x = n
    n_y = n // n_x
    most = max(n_x, n_y)

    def per_device(*args):
        args = args[:10] + tuple(w.reshape(1, -1) for w in args[10:])
        grads, weights, width = args[0:4], args[6:10], args[10].shape[1]
        blocks = [w.shape for w in weights]
        slices = blocks[0][0]
        slabs = [(b[0] // 2, b[1]) for b in blocks]
        lines = [(1, s[0]) for s in slabs[:3]] + [(1, slabs[3][1])]
        f32, bf16 = jnp.float32, jnp.bfloat16
        DMA = pltpu.SemaphoreType.DMA
        hops = max(most - 1, 1)
        turned = slabs[TURNED][0] * 6 // 256 * 16 if n_x == n_y == 2 else 0
        pieces = math.gcd(max(width // LANES, 1), m // 2)
        hbm = pl.BlockSpec(memory_space=pltpu.HBM)
        vmem = pl.BlockSpec(memory_space=pltpu.VMEM)
        out_shape = (
            [jax.ShapeDtypeStruct(g.shape[1:], bf16) for g in grads]
            + [jax.ShapeDtypeStruct(b, f32) for b in blocks]
            + [jax.ShapeDtypeStruct((2, n, 1, width), f32), jax.ShapeDtypeStruct((2, 1, width), f32)]
        )
        results = pl.pallas_call(
            functools.partial(kernel, n, m, n_x, n_y, turned),
            out_shape=[pltpu.VMEM(o.shape, o.dtype) for o in out_shape],
            in_specs=[hbm] * 12,
            out_specs=[vmem] * 10,
            scratch_shapes=(
                [pltpu.VMEM(g.shape[1:], f32) for g in grads]
                + [pltpu.VMEM(b, f32) for b in blocks] * 2
                + [pltpu.VMEM((2, hops, most) + s, bf16) for s in slabs] * 2
                + [pltpu.VMEM((2, hops) + s, bf16) for s in slabs] * 2
                + [pltpu.VMEM((2, hops, most + 1) + l, f32) for l in lines]
                + [pltpu.VMEM((2, hops, most) + l, f32) for l in lines]
                + [pltpu.VMEM((2, hops) + l, f32) for l in lines]
                + [
                    pltpu.VMEM((4, 2, slices), f32),
                    pltpu.VMEM((4, m, 2, slices), f32),
                    pltpu.VMEM((2, 1, (n + 1) * width), f32),
                    pltpu.VMEM((n, n + 1, 1, width // pieces), f32),
                    pltpu.VMEM((2 * pieces, n, 1, width // pieces), f32),
                    pltpu.VMEM((2, max(turned, 16)) + slabs[TURNED][1:], bf16),
                    pltpu.VMEM((2,) + lines[TURNED], f32),
                    DMA,
                    DMA((4,)),
                    DMA((4,)),
                    DMA,
                ]
                + [DMA((4,))] * 5
                + [DMA, DMA((4,)), DMA, DMA((2,)), DMA((3,))]
                + [pltpu.SemaphoreType.REGULAR] * 2
            ),
            compiler_params=pltpu.CompilerParams(
                collective_id=0, has_side_effects=True, vmem_limit_bytes=40 * 2**20
            ),
        )(*[pltpu.with_memory_space_constraint(v, pltpu.HBM) for v in args])
        done = pl.pallas_call(
            functools.partial(finish, n),
            out_shape=out_shape[:8]
            + [jax.ShapeDtypeStruct((n * width,), bf16)] * 2
            + [jax.ShapeDtypeStruct((width,), f32)] * 2,
            in_specs=[vmem] * 10,
            out_specs=[hbm] * 12,
            scratch_shapes=[pltpu.VMEM((n * width,), bf16)] * 2
            + [pltpu.VMEM((width,), f32)] * 2
            + [DMA((8,)), DMA((4,))],
            compiler_params=pltpu.CompilerParams(vmem_limit_bytes=2**20),
        )(*results)
        return tuple(done[0:4]) + tuple(done[8:10]) + tuple(done[4:8]) + tuple(done[10:12])

    in_specs = (
        (P("batch", None, "cols"),) * 3
        + (P("batch", "cols", None),)
        + (P("batch", None),) * 2
        + (P("batch", "cols"),) * 3
        + (P("cols", "batch"),)
        + (P("batch"),) * 2
    )
    out_specs = (
        (P(None, "cols"),) * 3
        + (P("cols", None),)
        + (P(),) * 2
        + (P("batch", "cols"),) * 3
        + (P("cols", "batch"),)
        + (P("batch"),) * 2
    )
    return jax.shard_map(per_device, mesh=mesh, in_specs=in_specs, out_specs=out_specs, check_vma=False)
```

```python
import functools
import math

import jax
import jax.numpy as jnp
from jax import lax
from jax.experimental import pallas as pl
from jax.experimental.pallas import tpu as pltpu
from jax.sharding import PartitionSpec as P

learn_rate = 0.4
LANES = 128
LOW, SPAN, TINY = 87.0, 175.0, 1e-30
TURNED = 2
ORDER = (
    ("F0", "W0", "W1", "W2", "W3", "F1", "F2", "A0", "S", "A1", "G2", "F3", "E", "N", "B0", "B1")
    + ("A2", "U0", "A3", "U1", "B2", "B3", "P0", "M", "U2", "U3", "P1", "P2", "P3")
)


def across(a, line, depth):
    return jnp.broadcast_to(line, (LANES, depth)).T if a < 3 else line


def blocks_of(a, columns):
    step = LANES if a < 3 else columns
    return [slice(start, start + step) for start in range(0, columns, step)]


def encode(a, value, code, unit):
    depth, columns = value.shape
    size = jnp.abs(value)
    if a < 3:
        size = functools.reduce(jnp.maximum, [size[:, block] for block in blocks_of(a, columns)]).T
    largest = jnp.maximum(jnp.max(size, axis=0, keepdims=True), TINY)
    unit[...] = largest * SPAN**-2
    gain = across(a, SPAN**2 / largest, depth)
    for block in blocks_of(a, columns):
        part = value[:, block]
        level = jnp.abs(part) * gain
        level = jnp.exp(level * lax.rsqrt(level + TINY) - LOW)
        code[:, block] = jnp.where(part < 0, -level, level).astype(jnp.bfloat16)


def decode(a, code, unit):
    rows, columns = code.shape
    scale = across(a, unit[...], unit.shape[1])[:rows]
    parts = []
    for block in blocks_of(a, columns):
        part = code[:, block].astype(jnp.float32)
        root = jnp.log(jnp.abs(part)) + LOW
        level = root * root * scale
        parts.append(jnp.where(part < 0, -level, level))
    return jnp.concatenate(parts, axis=1) if len(parts) > 1 else parts[0]


def drain(ref, sem):
    pltpu.make_async_copy(ref, ref, sem).wait()


def kernel(n, m, n_x, n_y, turned, *refs):
    grads, small_grads = refs[0:4], refs[4:6]
    weights, small_weights = refs[6:10], refs[10:12]
    copies = [refs[12].at[a] for a in range(3)] + [refs[13]]
    news = [refs[14].at[a] for a in range(3)] + [refs[15]]
    small_full, small_own = refs[16:18]
    scratch = refs[18:]
    full, total, own_weight = scratch[0:4], scratch[4:8], scratch[8:12]
    first_out, first_in = scratch[12:16], scratch[16:20]
    second_out, second_in = scratch[20:24], scratch[24:28]
    unit_out, first_unit, second_unit = scratch[28:32], scratch[32:36], scratch[36:40]
    squares, squares_in, small_hold, small_in, small_done = scratch[40:45]
    turned_in, turned_unit = scratch[45:47]
    (
        early_sem, load_sem, weight_sem, small_local,
        unit_first,
        first_recv, first_unit_recv, second_later, second_unit_recv,
        square_send, square_recv,
        small_arrived, done_sem, turned_sem, plane_sem, row_sem,
    ) = scratch[47:]
    sent = (early_sem,) + tuple(load_sem.at[a] for a in range(1, 4))
    back_recv, spread_recv = first_unit_recv, first_recv
    unit_sent = (unit_first,) + tuple(weight_sem.at[a] for a in range(1, 4))
    second_recv = (load_sem.at[0],) + tuple(second_later.at[a - 1] for a in range(1, 4))
    rate = n ** (-0.5)
    most = max(n_x, n_y)

    me = lax.axis_index("batch")
    col = lax.axis_index("cols")
    y, x = me // n_x, lax.rem(me, n_x)

    def spot(half, d_first, d_second):
        if half == 0:
            return lax.rem(y + d_second, n_y) * n_x + lax.rem(x + d_first, n_x)
        return lax.rem(y + d_first, n_y) * n_x + lax.rem(x + d_second, n_x)

    def extents(half):
        return (n_x, n_y) if half == 0 else (n_y, n_x)

    def piece(a, ref, chunk, half):
        rows, columns = total[a].shape
        depth = rows // 2
        if a < 3:
            start = pl.multiple_of(chunk * rows + half * depth, depth)
            return ref.at[pl.ds(start, depth), :]
        start = pl.multiple_of(chunk * columns, columns)
        return ref.at[pl.ds(half * depth, depth), pl.ds(start, columns)]

    def slots(a, ref, half):
        n_first, n_second = extents(half)
        return ref[a].at[half, pl.ds(0, n_first - 1), pl.ds(0, n_second)]

    odd = lax.rem(col, 2)
    row_col = col - odd
    plane_col = row_col + 1
    barrier = pltpu.get_barrier_semaphore()

    def greet(skip, **device):
        @pl.when(jnp.logical_not(skip))
        def _():
            pl.semaphore_signal(barrier, inc=1, device_id=device)

    neighbours = [spot(0, d, 0) for d in range(1, n_x)] + [spot(0, 0, d) for d in range(1, n_y)]
    for other in neighbours:
        pl.semaphore_signal(barrier, inc=1, device_id={"batch": other, "cols": plane_col})
    greet(odd == 1, batch=me, cols=plane_col)
    for d in range(0, m, 2):
        other = lax.rem(row_col + d, m)
        greet(other == col, batch=me, cols=other)

    def enter_plane():
        @pl.when(odd == 1)
        def _():
            pl.semaphore_wait(barrier, 2 * len(neighbours) + 1)
            pl.semaphore_signal(plane_sem, inc=1, device_id={"cols": row_col})

        @pl.when(odd == 0)
        def _():
            pl.semaphore_wait(plane_sem, 1)

    def enter_row():
        @pl.when(odd == 0)
        def _():
            pl.semaphore_wait(barrier, m - 1)
            pl.semaphore_signal(row_sem, inc=1, device_id={"cols": plane_col})

        @pl.when(odd == 1)
        def _():
            pl.semaphore_wait(row_sem, 1)

    early, rest = {}, []
    for half in range(2):
        n_first, n_second = extents(half)
        for d_first in range(n_first):
            for d_second in range(n_second):
                here = spot(half, d_first, d_second)
                first_sent = d_first > 0 and d_second == n_second - 1
                copy = pltpu.make_async_copy(
                    piece(0, grads[0].at[0], here, half),
                    piece(0, full[0], here, half),
                    early_sem if first_sent else load_sem.at[0],
                )
                if first_sent:
                    early[half, d_first] = copy
                else:
                    rest.append(copy)
    width = small_weights[0].shape[1]
    shares, chunk = small_done.shape[0], small_done.shape[3]
    per_array = shares // 2
    share = lax.rem(col, shares)
    smalls, weight_loads = [], []
    for i in range(2):
        smalls.append((small_grads[i], small_hold.at[i, :, pl.ds(0, n * width)]))
        smalls.append((small_weights[i], small_hold.at[i, :, pl.ds(n * width, width)]))
    for copy in early.values():
        copy.start()
    for copy in rest:
        copy.start()
    for a in range(1, 4):
        pltpu.make_async_copy(grads[a].at[0], full[a], load_sem.at[a]).start()
        if a == 1:
            for b in range(4):
                weight_loads.append(pltpu.make_async_copy(weights[b], own_weight[b], weight_sem.at[b]))
                weight_loads[b].start()
            for source, target in smalls:
                pltpu.make_async_copy(source, target, small_local).start()

    def load_rest(a):
        if a == 0:
            drain(full[0].at[pl.ds(0, len(rest) * (total[0].shape[0] // 2))], load_sem.at[0])
        else:
            drain(full[a], load_sem.at[a])

    entered, loaded, ready = [], set(), []

    def send(source, target, sem, arrival, device):
        pltpu.make_async_remote_copy(
            src_ref=source, dst_ref=target, send_sem=sem, recv_sem=arrival, device_id=device
        ).start()

    def send_turned(half):
        a, at, top = TURNED, (half, 0, 1), pl.ds(0, turned)
        turns = me == (1 if half == 0 else 2)
        std = {"batch": spot(half, 1, 0)}
        code = first_out[a].at[at + (top,)]
        below = pl.ds(turned, total[a].shape[0] // 2 - turned)
        send(first_out[a].at[at + (below,)], first_in[a].at[at + (below,)], sent[a], first_recv.at[a], std)

        @pl.when(jnp.logical_not(turns))
        def _():
            send(code, first_in[a].at[at + (top,)], sent[a], first_recv.at[a], std)

        @pl.when(turns)
        def _():
            far = {"batch": n - 1}
            send(unit_out[a].at[at], turned_unit.at[half], turned_sem.at[0], turned_sem.at[1], far)
            send(code, turned_in.at[half], sent[a], turned_sem.at[2], far)

    def add_turned(a):
        if a not in loaded:
            loaded.add(a)
            load_rest(a)
        if turned and a == TURNED:
            @pl.when(me == n - 1)
            def _():
                drain(turned_unit, turned_sem.at[1])
                drain(turned_in, turned_sem.at[2])
                for half in range(2):
                    own = piece(a, full[a], spot(half, 1, 0), half).at[pl.ds(0, turned)]
                    own[...] = own[...] + decode(a, turned_in.at[half], turned_unit.at[half])

        send_first(a, [0])

    def send_first(a, ds=None):
        if ds is None:
            ds = range(most - 1, -1 if a != TURNED else 0, -1)
        for d in ds:
            for half in range(2):
                n_first, n_second = extents(half)
                for d_first in range(1, n_first):
                    if d >= n_second:
                        continue
                    if a == 0 and d == n_second - 1:
                        if early:
                            drain(full[0].at[pl.ds(0, len(early) * (total[0].shape[0] // 2))], early_sem)
                            early.clear()
                    elif a not in loaded:
                        loaded.add(a)
                        load_rest(a)
                    at = (half, d_first - 1, d)
                    unit = unit_out[a].at[at]
                    encode(a, piece(a, full[a], spot(half, d_first, d), half)[...], first_out[a].at[at], unit)
                    to = {"batch": spot(half, d_first, 0)}
                    ready.append((unit, first_unit[a].at[at], unit_sent[a], first_unit_recv.at[a], to))
                    if turned and a == TURNED and d == 1:
                        ready.append((half,))
                    else:
                        ready.append((first_out[a].at[at], first_in[a].at[at], sent[a], first_recv.at[a], to))
            if not entered:
                entered.append(True)
                enter_plane()
            for item in ready:
                send_turned(*item) if len(item) == 1 else send(*item)
            ready.clear()

    def send_small():
        drain(small_hold, small_local)
        start = lax.rem(share, per_array) * chunk
        for k in range(n + 1):
            small_in[me, k] = small_hold[share // per_array, :, pl.ds(pl.multiple_of(k * width + start, chunk), chunk)]
        for d in range(1, n):
            send(small_in.at[me], small_in.at[me], small_local, small_arrived, {"batch": lax.rem(me + d, n)})

    def row_squares(a, value):
        value = value * value
        if a == 3:
            return jnp.sum(value, axis=0, keepdims=True)
        folded = value[:, :LANES]
        for start in range(LANES, value.shape[1], LANES):
            folded = folded + value[:, start : start + LANES]
        return jnp.sum(folded.T, axis=0, keepdims=True)

    def weigh(a):
        weight_loads[a].wait()
        squares[a, 0:1] = row_squares(a, own_weight[a][...])

    def drain_first(a, ref, sem):
        if n_x == n_y:
            drain(ref[a], sem)
        else:
            for half in range(2):
                if extents(half)[0] > 1:
                    drain(slots(a, ref, half), sem)

    def add_first(a):
        if a not in loaded:
            loaded.add(a)
            load_rest(a)
        drain_first(a, first_unit, first_unit_recv.at[a])
        if turned and a == TURNED:
            @pl.when(me == 0)
            def _():
                drain(full[a].at[pl.ds(0, total[a].shape[0] - turned)], first_recv.at[a])

            @pl.when(me != 0)
            def _():
                drain_first(a, first_in, first_recv.at[a])
        else:
            drain_first(a, first_in, first_recv.at[a])
        for d_second in range(most - 1, -1, -1):
            for half in range(2):
                n_first, n_second = extents(half)
                if d_second >= n_second:
                    continue
                own = piece(a, full[a], spot(half, 0, d_second), half)
                value = own[...]
                for d_first in range(1, n_first):
                    at = (half, d_first - 1, d_second)
                    before, value = value, value + decode(a, first_in[a].at[at], first_unit[a].at[at])
                    if turned and a == TURNED and d_second == 1:
                        top = jnp.where(me == 0, before[:turned], value[:turned])
                        value = jnp.concatenate([top, value[turned:]], axis=0)
                if d_second == 0:
                    own[...] = value
                    continue
                at = (half, d_second - 1)
                unit = unit_out[a].at[at + (most,)]
                encode(a, value, second_out[a].at[at], unit)
                to = {"batch": spot(half, 0, d_second)}
                send(unit, second_unit[a].at[at], unit_sent[a], second_unit_recv.at[a], to)
                send(second_out[a].at[at], second_in[a].at[at], sent[a], second_recv[a], to)

    def used_second(a, ref):
        if n_x == n_y:
            return ref[a]
        half = 0 if n_y > 1 else 1
        return ref[a].at[half, pl.ds(0, extents(half)[1] - 1)]

    def add_second(a):
        drain(used_second(a, second_unit), second_unit_recv.at[a])
        drain(used_second(a, second_in), second_recv[a])
        depth = total[a].shape[0] // 2
        for half in range(2):
            value = piece(a, full[a], me, half)[...]
            for d_second in range(1, extents(half)[1]):
                at = (half, d_second - 1)
                value = value + decode(a, second_in[a].at[at], second_unit[a].at[at])
            total[a][half * depth : (half + 1) * depth] = value * rate
        squares[a, 1:2] = row_squares(a, total[a][...])
        squares_in[a, col] = squares[a]
        for d in range(1, m):
            send(squares.at[a], squares_in.at[a, col], square_send, square_recv.at[a], {"cols": lax.rem(col + d, m)})

    def send_spread(a, half, d_second):
        n_first, n_second = extents(half)
        slab = piece(a, copies[a], spot(half, 0, n_second - d_second), half)
        for d_first in range(1, n_first):
            send(slab, slab, sent[a], spread_recv.at[a], {"batch": spot(half, d_first, 0)})

    def update(a):
        drain(squares_in.at[a, pl.ds(0, m - 1)], square_recv.at[a])
        both = squares_in[a, 0]
        for d in range(1, m):
            both = both + squares_in[a, d]
        ratio = learn_rate * (jnp.sqrt(both[0:1]) * lax.rsqrt(both[1:2] + 1e-06))
        rows, columns = total[a].shape
        if a < 3:
            ratio = jnp.broadcast_to(ratio, (LANES, rows)).T
            for start in range(0, columns, LANES):
                block = slice(start, start + LANES)
                news[a][:, block] = own_weight[a][:, block] - total[a][:, block] * ratio
        else:
            news[a][...] = own_weight[a][...] - total[a][...] * ratio
        depth = rows // 2
        for half in range(2):
            piece(a, copies[a], me, half)[...] = news[a][half * depth : (half + 1) * depth].astype(jnp.bfloat16)
        for half in range(2):
            slab = piece(a, copies[a], me, half)
            for d_second in range(1, extents(half)[1]):
                send(slab, slab, sent[a], back_recv.at[a], {"batch": spot(half, 0, d_second)})
        for half in range(2):
            send_spread(a, half, 0)

    def pass_on(a):
        drain(used_second(a, second_in), back_recv.at[a])
        for half in range(2):
            for d_second in range(1, extents(half)[1]):
                send_spread(a, half, d_second)

    def update_small():
        drain(small_in.at[pl.ds(0, n - 1)], small_arrived)
        for k in range(n):
            value = small_in[0, k]
            for j in range(1, n):
                value = value + small_in[j, k]
            small_done[share, k] = small_in[k, n] - learn_rate * (value * rate)
        for d in range(1, shares):
            to = {"cols": col - share + lax.rem(share + d, shares)}
            send(small_done.at[share], small_done.at[share], done_sem.at[0], done_sem.at[1], to)

    def gather_small():
        drain(small_done.at[pl.ds(0, shares - 1)], done_sem.at[1])
        for i in range(2):
            for k in range(n):
                for j in range(per_array):
                    small_full[i, k, :, j * chunk : (j + 1) * chunk] = small_done[i * per_array + j, k]
            small_own[i] = small_full[i, me]

    steps = dict(
        F=send_first, G=add_turned, S=send_small, W=weigh, A=add_first, B=add_second, U=update, P=pass_on
    )
    steps.update(N=update_small, M=gather_small, E=enter_row)
    for step in ORDER:
        steps[step[0]](*map(int, step[1:]))
    drain(small_in.at[pl.ds(0, n - 1)], small_local)
    drain(small_done.at[pl.ds(0, shares - 1)], done_sem.at[0])
    drain(squares_in.at[:, pl.ds(0, m - 1)], square_send)
    for a in range(4):
        drain(unit_out[a], unit_sent[a])
    if turned:
        @pl.when(jnp.logical_or(me == 1, me == 2))
        def _():
            drain(turned_unit.at[0], turned_sem.at[0])
    for a in range(4):
        rows, columns = full[a].shape
        slabs = 2 * sum((extents(h)[0] - 1) * extents(h)[1] + extents(h)[1] - 1 for h in range(2))
        gone = slabs * (total[a].shape[0] // 2) * total[a].shape[1] // 2
        drain(full[a].at[pl.ds(0, gone // columns)], sent[a])
        drain_first(a, first_in, spread_recv.at[a])


def finish(n, *refs):
    copies, copy_mixed, news, new_mixed, full, own = refs[0:6]
    outs, small_copies, small_news = refs[6:14], refs[14:16], refs[16:18]
    copy_rows, new_rows, sem, small_sem = refs[18:20], refs[20:22], refs[22], refs[23]
    for a in range(3):
        pltpu.make_async_copy(copies.at[a], outs[a], sem.at[0]).start()
    moves = [pltpu.make_async_copy(copy_mixed, outs[3], sem.at[1])]
    moves.append(pltpu.make_async_copy(new_mixed, outs[7], sem.at[2]))
    for move in moves:
        move.start()
    for a in range(3):
        pltpu.make_async_copy(news.at[a], outs[4 + a], sem.at[3]).start()
    width = full.shape[-1]
    for i in range(2):
        for j in range(n):
            copy_rows[i][j * width : (j + 1) * width] = full[i, j, 0].astype(jnp.bfloat16)
        new_rows[i][...] = own[i, 0]
    for i in range(2):
        moves.append(pltpu.make_async_copy(copy_rows[i], small_copies[i], small_sem.at[i]))
        moves.append(pltpu.make_async_copy(new_rows[i], small_news[i], small_sem.at[2 + i]))
    for move in moves[2:]:
        move.start()
    drain(copies, sem.at[0])
    drain(news, sem.at[3])
    for move in moves:
        move.wait()


def solution(mesh):
    n, m = mesh.shape["batch"], mesh.shape["cols"]
    n_x = math.isqrt(n)
    if n_x * n_x != n:
        n_x = n
    n_y = n // n_x
    most = max(n_x, n_y)

    def per_device(*args):
        args = args[:10] + tuple(w.reshape(1, -1) for w in args[10:])
        grads, weights, width = args[0:4], args[6:10], args[10].shape[1]
        blocks = [w.shape for w in weights]
        slices = blocks[0][0]
        slabs = [(b[0] // 2, b[1]) for b in blocks]
        lines = [(1, s[0]) for s in slabs[:3]] + [(1, slabs[3][1])]
        f32, bf16 = jnp.float32, jnp.bfloat16
        DMA = pltpu.SemaphoreType.DMA
        hops = max(most - 1, 1)
        turned = slabs[TURNED][0] * 6 // 256 * 16 if n_x == n_y == 2 else 0
        pieces = math.gcd(max(width // LANES, 1), m // 2)
        hbm = pl.BlockSpec(memory_space=pltpu.HBM)
        vmem = pl.BlockSpec(memory_space=pltpu.VMEM)
        out_shape = (
            [jax.ShapeDtypeStruct(g.shape[1:], bf16) for g in grads]
            + [jax.ShapeDtypeStruct(b, f32) for b in blocks]
            + [jax.ShapeDtypeStruct((2, n, 1, width), f32), jax.ShapeDtypeStruct((2, 1, width), f32)]
        )
        shapes = [o.shape for o in out_shape]
        grouped = [((3,) + shapes[0], bf16), (shapes[3], bf16), ((3,) + shapes[4], f32), (shapes[7], f32)]
        grouped += [(s, f32) for s in shapes[8:]]
        results = pl.pallas_call(
            functools.partial(kernel, n, m, n_x, n_y, turned),
            out_shape=[pltpu.VMEM(s, t) for s, t in grouped],
            in_specs=[hbm] * 12,
            out_specs=[vmem] * 6,
            scratch_shapes=(
                [pltpu.VMEM(g.shape[1:], f32) for g in grads]
                + [pltpu.VMEM(b, f32) for b in blocks] * 2
                + [pltpu.VMEM((2, hops, most) + s, bf16) for s in slabs] * 2
                + [pltpu.VMEM((2, hops) + s, bf16) for s in slabs] * 2
                + [pltpu.VMEM((2, hops, most + 1) + l, f32) for l in lines]
                + [pltpu.VMEM((2, hops, most) + l, f32) for l in lines]
                + [pltpu.VMEM((2, hops) + l, f32) for l in lines]
                + [
                    pltpu.VMEM((4, 2, slices), f32),
                    pltpu.VMEM((4, m, 2, slices), f32),
                    pltpu.VMEM((2, 1, (n + 1) * width), f32),
                    pltpu.VMEM((n, n + 1, 1, width // pieces), f32),
                    pltpu.VMEM((2 * pieces, n, 1, width // pieces), f32),
                    pltpu.VMEM((2, max(turned, 16)) + slabs[TURNED][1:], bf16),
                    pltpu.VMEM((2,) + lines[TURNED], f32),
                    DMA,
                    DMA((4,)),
                    DMA((4,)),
                    DMA,
                ]
                + [DMA, DMA((4,)), DMA((4,)), DMA((3,)), DMA((4,))]
                + [DMA, DMA((4,)), DMA, DMA((2,)), DMA((3,))]
                + [pltpu.SemaphoreType.REGULAR] * 2
            ),
            compiler_params=pltpu.CompilerParams(
                collective_id=0, has_side_effects=True, vmem_limit_bytes=40 * 2**20
            ),
        )(*[pltpu.with_memory_space_constraint(v, pltpu.HBM) for v in args])
        done = pl.pallas_call(
            functools.partial(finish, n),
            out_shape=out_shape[:8]
            + [jax.ShapeDtypeStruct((n * width,), bf16)] * 2
            + [jax.ShapeDtypeStruct((width,), f32)] * 2,
            in_specs=[vmem] * 6,
            out_specs=[hbm] * 12,
            scratch_shapes=[pltpu.VMEM((n * width,), bf16)] * 2
            + [pltpu.VMEM((width,), f32)] * 2
            + [DMA((4,)), DMA((4,))],
            compiler_params=pltpu.CompilerParams(vmem_limit_bytes=2**20),
        )(*results)
        return tuple(done[0:4]) + tuple(done[8:10]) + tuple(done[4:8]) + tuple(done[10:12])

    in_specs = (
        (P("batch", None, "cols"),) * 3
        + (P("batch", "cols", None),)
        + (P("batch", None),) * 2
        + (P("batch", "cols"),) * 3
        + (P("cols", "batch"),)
        + (P("batch"),) * 2
    )
    out_specs = (
        (P(None, "cols"),) * 3
        + (P("cols", None),)
        + (P(),) * 2
        + (P("batch", "cols"),) * 3
        + (P("cols", "batch"),)
        + (P("batch"),) * 2
    )
    return jax.shard_map(per_device, mesh=mesh, in_specs=in_specs, out_specs=out_specs, check_vma=False)
```
